256 devices in a mesh: dp: 32 (over z_lo, x, core), mp: 8 (over z_hi, y).
Axes of the slice: x: 4, y: 4, z: 8 (z_hi: 2, z_lo: 4; z = z_hi * 4 + z_lo), core: 2. Of those that a mesh axis runs over, the one named last changes fastest.
Arguments:
- queries: bfloat16 [24576, 1024], P('dp', 'mp'), may hold values from -3 to 3
- passages: bfloat16 [24576, 1024], P('dp', 'mp'), may hold values from -3 to 3
- positive: int32 [24576], P('dp'), may hold values from 0 to 24575
Outputs:
- grad_queries: bfloat16 [24576, 1024], P('dp', 'mp')
- grad_passages: bfloat16 [24576, 1024], P('dp', 'mp')
The draws below stay inside these ranges and needn't reach their ends.
All inputs are finite; a program needn't handle non-finite values.
Results may differ from the reference program's by a relative error of at most 0.0034.
Values may be sent and summed in bfloat16 or wider, within the bound.
No kernel may reach another device: no remote copies, remote signals or barrier semaphores. Data moves between devices by JAX's collectives and lax.ppermute only.
A program may use at most 128 MiB of HBM per device.

```python
import math
import jax
import jax.numpy as jnp
from jax import lax

D = 1024
PAIRS = 24576


def paired_draw(key):
    inner = jax.random.fold_in(key, 11)
    first_key, second_key, third_key = jax.random.split(inner, 3)
    query_vals = jnp.clip(jax.random.normal(first_key, (PAIRS, D), jnp.float32), -3.0, 3.0)
    passage_vals = jnp.clip(jax.random.normal(second_key, (PAIRS, D), jnp.float32), -3.0, 3.0)
    return (query_vals.astype(jnp.bfloat16), passage_vals.astype(jnp.bfloat16))


def draw_queries(key, part):
    return paired_draw(key)[0]


def draw_passages(key, part):
    return paired_draw(key)[1]


def place_ends(drawn, key, least, high):
    shape = drawn.shape
    place = [jax.random.randint(jax.random.fold_in(key, axis), (), 0, shape[axis]) for axis in range(len(shape))]
    drawn = drawn.at[tuple(place)].set(least)
    longest = shape.index(max(shape))
    place[longest] = (place[longest] + 1) % shape[longest]
    return drawn.at[tuple(place)].set(high)


def setup_inputs(seed: int = 0) -> dict:
    key_of = jax.random.split(jax.random.key(seed), 4)
    return {
        "queries": draw_queries(jax.random.fold_in(key_of[3], 71), 0),
        "passages": draw_passages(jax.random.fold_in(key_of[3], 71), 0),
        "positive": place_ends(jax.random.randint(key_of[2], (PAIRS,), 0, PAIRS), jax.random.fold_in(key_of[2], 1), 0, PAIRS - 1).astype(jnp.int32),
    }


def reference(queries, passages, positive):
    logit_scale = 3.0 / math.sqrt(D)
    block_rows = math.gcd(PAIRS, 512)
    block_count = PAIRS // block_rows
    query_blocks = queries.reshape(block_count, block_rows, D)
    target_blocks = positive.reshape(block_count, block_rows)
    column_ids = jnp.arange(PAIRS, dtype=jnp.int32)

    def one_block(carried, inputs):
        query_rows, targets = inputs
        scores = jnp.dot(query_rows, passages.T, preferred_element_type=jnp.float32) * logit_scale
        highest = lax.optimization_barrier(jnp.max(scores, axis=1))
        log_total = highest + jnp.log(lax.optimization_barrier(jnp.sum(jnp.exp(scores - highest[:, None]), axis=1)))
        onehot = (column_ids[None, :] == targets[:, None]).astype(jnp.float32)
        softmax_grad = (jnp.exp(scores - log_total[:, None]) - onehot).astype(jnp.bfloat16)
        query_grad = jnp.dot(softmax_grad, passages, preferred_element_type=jnp.float32).astype(jnp.bfloat16)
        carried = carried + jnp.dot(softmax_grad.T, query_rows, preferred_element_type=jnp.float32)
        return (carried, query_grad)
    start_grad = jnp.zeros((PAIRS, D), jnp.float32)
    passage_total, query_grads = lax.scan(one_block, start_grad, (query_blocks, target_blocks))
    return (query_grads.reshape(PAIRS, D), passage_total.astype(jnp.bfloat16))
```

```python
import math

import jax
import jax.numpy as jnp
from jax import lax
from jax.sharding import Mesh
from jax.sharding import PartitionSpec as P

WIDTH = ("zh", "y")
PLANE = ("x", "y")
F32, BF16 = jnp.float32, jnp.bfloat16


def along_z(array, step):
    place = lambda z: (z % 4) * 2 + z // 4
    return lax.ppermute(array, ("zl", "zh"), [(place(z), place((z + step) % 8)) for z in range(8)])


def other_core(array):
    return lax.ppermute(array, "c", [(0, 1), (1, 0)])


def along_x(array, step):
    return lax.ppermute(array, "x", [(k, (k + step) % 4) for k in range(4)])


def to_plane(array):
    copies = jnp.broadcast_to(array[None], (16, *array.shape))
    return lax.all_to_all(copies, PLANE, 0, 0, tiled=True)


def local(queries, passages, positive):
    rows, width = queries.shape
    part = rows // 8
    full = width * 8
    x, y, c = (lax.axis_index(a) for a in ("x", "y", "c"))
    zl, zh = lax.axis_index("zl"), lax.axis_index("zh")
    z = zh * 4 + zl

    both = jnp.concatenate([queries.reshape(8, part, width), passages.reshape(8, part, width)], 1)
    both = lax.all_to_all(both, WIDTH, 0, 0, tiled=True)
    both = both.transpose(1, 0, 2).reshape(2 * part, full)
    query_part, passage_part = both[:part], both[part:]

    block_queries = to_plane(query_part).reshape(16 * part, full)
    rings = [passage_part] + [along_z(passage_part, d) for d in range(1, 8)]
    own = jnp.concatenate(rings)
    block_passages = jnp.concatenate([own, other_core(own)])

    mine = lax.dynamic_slice(positive, (zh * 4 * part,), (4 * part,))
    nearby = jnp.stack([mine] + [along_x(mine, d) for d in range(1, 4)])
    order = (x - jnp.arange(4)) % 4
    targets = jnp.take(nearby, order, axis=0).reshape(16 * part)

    source_z = (z - jnp.arange(8)) % 8
    source_c = jnp.stack([c, 1 - c])
    group = ((source_z % 4) * 4 + x)[None, :] * 2 + source_c[:, None]
    first = group * rows + ((source_z // 4) * 4 + y)[None, :] * part
    ids = (first[:, :, None] + jnp.arange(part)).reshape(16 * part).astype(jnp.int32)

    scale = 3.0 / math.sqrt(full)
    scores = (
        lax.dot_general(
            block_queries, block_passages, (((1,), (1,)), ((), ())), preferred_element_type=F32
        )
        * scale
    )
    peak = jnp.max(scores, axis=1)
    total = jnp.sum(jnp.exp(scores - peak[:, None]), axis=1)
    stats = to_plane(jnp.stack([peak, total]))
    highest = jnp.max(stats[:, 0], axis=0)
    log_total = highest + jnp.log(jnp.sum(stats[:, 1] * jnp.exp(stats[:, 0] - highest), axis=0))
    onehot = (ids[None, :] == targets[:, None]).astype(F32)
    softmax_grad = (jnp.exp(scores - log_total[:, None]) - onehot).astype(BF16)

    passage_terms = lax.dot_general(
        softmax_grad, block_queries, (((0,), (0,)), ((), ())), preferred_element_type=F32
    )
    half = 8 * part
    pair = passage_terms[:half] + other_core(passage_terms[half:])
    pair = pair.astype(BF16).reshape(8, part, full)

    query_terms = jnp.dot(softmax_grad, block_passages, preferred_element_type=F32).astype(BF16)
    query_terms = lax.all_to_all(query_terms.reshape(16, part, full), PLANE, 0, 0, tiled=True)
    grad_queries = jnp.sum(query_terms.astype(F32), axis=0).astype(BF16)

    grad_passages = pair[0].astype(F32)
    for d in range(1, 8):
        grad_passages = grad_passages + along_z(pair[d], -d).astype(F32)
    grad_passages = grad_passages.astype(BF16)

    both = jnp.concatenate([grad_queries, grad_passages]).reshape(2 * part, 8, width)
    both = lax.all_to_all(both.transpose(1, 0, 2), WIDTH, 0, 0, tiled=True)
    return both[:, :part].reshape(rows, width), both[:, part:].reshape(rows, width)


def solution(mesh):
    finer = Mesh(mesh.devices.reshape(4, 4, 2, 2, 4), ("zl", "x", "c", "zh", "y"))
    groups = ("zl", "x", "c")
    return jax.shard_map(
        local,
        mesh=finer,
        in_specs=(P(groups, WIDTH), P(groups, WIDTH), P(groups)),
        out_specs=(P(groups, WIDTH), P(groups, WIDTH)),
        check_vma=False,
    )
```

```python
import functools
import math

import jax
import jax.numpy as jnp
from jax import lax
from jax.experimental import pallas as pl
from jax.experimental.pallas import tpu as pltpu
from jax.sharding import Mesh
from jax.sharding import PartitionSpec as P

WIDTH = ("zh", "y")
PLANE = ("x", "y")
F32, BF16 = jnp.float32, jnp.bfloat16
INTERPRET = False


def along_z(array, step):
    place = lambda z: (z % 4) * 2 + z // 4
    return lax.ppermute(array, ("zl", "zh"), [(place(z), place((z + step) % 8)) for z in range(8)])


def swapped(array, axis):
    return lax.ppermute(array, axis, [(0, 1), (1, 0)])


def to_plane(array):
    copies = jnp.broadcast_to(array[None], (16, *array.shape))
    return lax.all_to_all(copies, PLANE, 0, 0, tiled=True)


def dot(a, b, dims):
    return lax.dot_general(a, b, (dims, ((), ())), preferred_element_type=F32)


def ring_gather(piece):
    half = piece.shape[0] // 2
    down, up = [piece], [piece]
    for _ in range(3):
        down.append(along_z(down[-1], 1))
        up.append(along_z(up[-1], -1))
    far = jnp.concatenate([along_z(down[3][:half], 1), along_z(up[3][half:], -1)])
    return jnp.concatenate([*down, far, up[3], up[2], up[1]])


def kernel(body, grid, in_specs, out_specs, out_shape, flops):
    return pl.pallas_call(
        body,
        grid_spec=pltpu.PrefetchScalarGridSpec(
            num_scalar_prefetch=1,
            grid=(grid,),
            in_specs=in_specs,
            out_specs=out_specs,
        ),
        out_shape=out_shape,
        compiler_params=pltpu.CompilerParams(
            dimension_semantics=("arbitrary",), vmem_limit_bytes=56 * 2**20
        ),
        cost_estimate=pl.CostEstimate(flops=flops, transcendentals=0, bytes_accessed=flops // 512),
        interpret=INTERPRET,
    )


def spec(block, index):
    return pl.BlockSpec(block, lambda i, s: index(i))


def whole(shape):
    return spec(shape, lambda i: (0,) * len(shape))


def score_body(s, pieces, own, other, queries, passages, scores, peak, total, *, scale):
    quarter, wide = own.shape[1], own.shape[2]
    width = pieces.shape[3]

    @pl.when(pl.program_id(0) == 0)
    def _():
        for c, part in enumerate((own, other)):
            for d in range(4):
                for h in range(2):
                    at = (c * 4 + d) * quarter
                    piece = part[jnp.where((s[0] >= d) == (h == 0), d, d + 4)]
                    passages[at : at + quarter, h * wide : (h + 1) * wide] = piece

    for y in range(4):
        for h in range(2):
            at = (h * 4 + y) * width
            queries[:, at : at + width] = pieces[y, h]
    block = 2 * quarter
    top = None
    for k in range(4):
        part = dot(passages[k * block : (k + 1) * block], queries[...], ((1,), (1,))) * scale
        scores[k * block : (k + 1) * block] = part
        high = jnp.max(part, axis=0, keepdims=True)
        top = high if top is None else jnp.maximum(top, high)
    summed = 0.0
    for k in range(4):
        part = scores[k * block : (k + 1) * block]
        summed += jnp.sum(jnp.exp(part - top), axis=0, keepdims=True)
    peak[0] = top
    total[0] = summed


def scored(scalars, pieces, own, other):
    _, _, rows, width = pieces.shape
    quarter = own.shape[1]
    full, count = 8 * width, 4 * rows
    row = jax.ShapeDtypeStruct((4, 1, rows), F32)
    return kernel(
        functools.partial(score_body, scale=3.0 / math.sqrt(full)),
        4,
        [
            spec((4, 2, rows, width), lambda i: (i, 0, 0, 0)),
            whole(own.shape),
            whole(other.shape),
        ],
        [
            spec((rows, full), lambda i: (i, 0)),
            whole((8 * quarter, full)),
            spec((8 * quarter, rows), lambda i: (0, i)),
            spec((1, 1, rows), lambda i: (i, 0, 0)),
            spec((1, 1, rows), lambda i: (i, 0, 0)),
        ],
        [
            jax.ShapeDtypeStruct((count, full), BF16),
            jax.ShapeDtypeStruct((8 * quarter, full), BF16),
            jax.ShapeDtypeStruct((8 * quarter, count), F32),
            row,
            row,
        ],
        2 * count * 8 * quarter * full,
    )(scalars, pieces, own, other)


def softmax_part(s, scores, log_total, targets, first):
    quarter = scores.shape[0] if scores.ndim == 2 else 0
    ids = s[1 + first] + lax.broadcasted_iota(jnp.int32, (quarter, 1), 0)
    hit = (ids == targets).astype(F32)
    return (jnp.exp(scores - log_total) - hit).astype(BF16)


def other_body(s, scores, log_total, targets, queries, grad, terms):
    quarter = scores.shape[0] // 2
    for k in range(2):
        rows = slice(k * quarter, (k + 1) * quarter)
        first = 4 + 2 * pl.program_id(0) + k
        grad[rows] = softmax_part(s, scores[rows], log_total[...], targets[...], first)
    terms[...] = dot(grad[...], queries[...], ((1,), (0,)))


def other_terms(scalars, scores, log_total, targets, queries):
    count, full = queries.shape
    block = scores.shape[0] // 4
    return kernel(
        other_body,
        2,
        [
            spec((block, count), lambda i: (i + 2, 0)),
            whole(log_total.shape),
            whole(targets.shape),
            whole(queries.shape),
        ],
        [spec((block, count), lambda i: (i, 0)), spec((block, full), lambda i: (i, 0))],
        [
            jax.ShapeDtypeStruct((2 * block, count), BF16),
            jax.ShapeDtypeStruct((2 * block, full), F32),
        ],
        2 * count * 2 * block * full,
    )(scalars, scores, log_total, targets, queries)


def query_body(s, scores, log_total, targets, other, passages, grad, out):
    half, width = scores.shape[0], out.shape[3]
    quarter = half // 4
    for d in range(4):
        rows = slice(d * quarter, (d + 1) * quarter)
        grad[rows] = softmax_part(s, scores[rows], log_total[...], targets[...], d)
    terms = dot(grad[...], passages[:half], ((0,), (0,)))
    terms += dot(other[...], passages[half:], ((0,), (0,)))
    terms = terms.astype(BF16)
    for y in range(4):
        for h in range(2):
            at = (h * 4 + y) * width
            out[y, h] = terms[:, at : at + width]


def query_terms(scalars, scores, log_total, targets, other, passages):
    count, full = scores.shape[1], passages.shape[1]
    half, rows = scores.shape[0] // 2, count // 4
    return kernel(
        query_body,
        4,
        [
            spec((half, rows), lambda i: (0, i)),
            spec((1, rows), lambda i: (0, i)),
            spec((1, rows), lambda i: (0, i)),
            spec((half, rows), lambda i: (0, i)),
            whole(passages.shape),
        ],
        [
            spec((half, rows), lambda i: (0, i)),
            spec((4, 2, rows, full // 8), lambda i: (i, 0, 0, 0)),
        ],
        [
            jax.ShapeDtypeStruct((half, count), BF16),
            jax.ShapeDtypeStruct((16, 2, rows, full // 8), BF16),
        ],
        2 * count * 2 * half * full,
    )(scalars, scores, log_total, targets, other, passages)


def own_body(s, grad, queries, theirs, near, far):
    quarter, wide = near.shape[1], near.shape[2]
    pair = dot(grad[...], queries[...], ((1,), (0,))) + theirs[...]
    for k in range(2):
        here = s[0] >= 2 * pl.program_id(0) + k
        left = pair[k * quarter : (k + 1) * quarter, :wide].astype(BF16)
        right = pair[k * quarter : (k + 1) * quarter, wide:].astype(BF16)
        near[k] = jnp.where(here, left, right)
        far[k] = jnp.where(here, right, left)


def own_terms(scalars, grad, queries, theirs):
    count, full = queries.shape
    block = grad.shape[0] // 2
    piece = (2, block // 2, full // 2)
    shape = jax.ShapeDtypeStruct((4, block // 2, full // 2), BF16)
    return kernel(
        own_body,
        2,
        [
            spec((block, count), lambda i: (i, 0)),
            whole(queries.shape),
            spec((block, full), lambda i: (i, 0)),
        ],
        [spec(piece, lambda i: (i, 0, 0)), spec(piece, lambda i: (i, 0, 0))],
        [shape, shape],
        2 * count * 2 * block * full,
    )(scalars, grad, queries, theirs)


def sum_body(s, terms, *refs):
    *parts, queries, passages = refs
    total = terms[0].astype(F32)
    for k in range(1, 16):
        total += terms[k].astype(F32)
    queries[...] = total.astype(BF16)
    total = parts[0][...].astype(F32)
    for part in parts[1:]:
        total += part[...].astype(F32)
    passages[0] = total.astype(BF16)


def summed(scalars, terms, parts):
    _, _, rows, width = terms.shape
    quarter = parts[0].shape[0]
    return kernel(
        sum_body,
        4,
        [spec((16, 2, rows // 4, width), lambda i: (0, 0, i, 0))]
        + [spec((quarter, width), lambda i: (0, i))] * 8,
        [
            spec((2, rows // 4, width), lambda i: (0, i, 0)),
            spec((1, quarter, width), lambda i: (i, 0, 0)),
        ],
        [
            jax.ShapeDtypeStruct((2, rows, width), BF16),
            jax.ShapeDtypeStruct((4, quarter, width), BF16),
        ],
        64 * rows * width,
    )(scalars, terms, *parts)


def step(queries, passages, positive):
    rows, width = queries.shape
    half, quarter = rows // 2, rows // 4
    x, y, c = (lax.axis_index(a) for a in ("x", "y", "c"))
    zl, zh = lax.axis_index("zl"), lax.axis_index("zh")

    kept = lax.dynamic_slice(queries, (zh * half, 0), (half, width))
    sent = lax.dynamic_slice(queries, ((1 - zh) * half, 0), (half, width))
    pieces = to_plane(jnp.stack([kept, swapped(sent, "zh")]))

    passage_part = lax.all_to_all(passages.reshape(4, quarter, width), "y", 0, 0, tiled=True)
    passage_part = passage_part.transpose(1, 0, 2).reshape(quarter, 4 * width)
    own = ring_gather(passage_part).reshape(8, quarter, 4 * width)
    other = swapped(own, "c")

    source_c = jnp.stack([c, 1 - c])
    group = (((zl - jnp.arange(4)) % 4) * 4 + x)[None, :] * 2 + source_c[:, None]
    first = (group * rows + y * quarter).reshape(8)
    scalars = jnp.concatenate([zl[None], first]).astype(jnp.int32)

    block_queries, block_passages, scores, peak, total = scored(scalars, pieces, own, other)
    mine = lax.dynamic_slice(positive, (zh * half,), (half,)).astype(F32)
    stats = to_plane(jnp.concatenate([peak[:, 0], total[:, 0], mine[None]]))
    peaks, totals = stats[:, :4], stats[:, 4:8]
    targets = stats[:, 8].reshape(4, 4, half)[:, 0].reshape(1, 4 * half).astype(jnp.int32)
    highest = jnp.max(peaks, axis=0)
    log_total = highest + jnp.log(jnp.sum(totals * jnp.exp(peaks - highest), axis=0))
    log_total = log_total.reshape(1, 4 * half)

    other_grad, sent = other_terms(scalars, scores, log_total, targets, block_queries)
    theirs = swapped(sent, "c")
    own_grad, terms = query_terms(scalars, scores, log_total, targets, other_grad, block_passages)
    terms = lax.all_to_all(terms, PLANE, 0, 0, tiled=True)
    near, far = own_terms(scalars, own_grad, block_queries, theirs)

    parts = [near[0], along_z(far[0], -4)]
    for d in (3, 1, 2):
        parts += [along_z(near[d], -d), along_z(far[d], -d - 4)]
    grad_queries, grad_passages = summed(scalars, terms, parts)
    grad_passages = lax.all_to_all(grad_passages, "y", 0, 0, tiled=True).reshape(rows, width)
    kept, received = grad_queries[0], swapped(grad_queries[1], "zh")
    grad_queries = jnp.where(
        zh == 0, jnp.concatenate([kept, received]), jnp.concatenate([received, kept])
    )
    return grad_queries, grad_passages


def solution(mesh):
    finer = Mesh(mesh.devices.reshape(4, 4, 2, 2, 4), ("zl", "x", "c", "zh", "y"))
    groups = ("zl", "x", "c")
    return jax.shard_map(
        step,
        mesh=finer,
        in_specs=(P(groups, WIDTH), P(groups, WIDTH), P(groups)),
        out_specs=(P(groups, WIDTH), P(groups, WIDTH)),
        check_vma=False,
    )
```

```python
import math

import jax
import jax.numpy as jnp
from jax import lax
from jax.experimental import pallas as pl
from jax.experimental.pallas import tpu as pltpu
from jax.sharding import Mesh
from jax.sharding import PartitionSpec as P

WIDTH = ("zh", "y")
PLANE = ("x", "y")
F32, BF16 = jnp.float32, jnp.bfloat16
INTERPRET = False
SDS = jax.ShapeDtypeStruct


def along_z(array, step):
    place = lambda z: (z % 4) * 2 + z // 4
    return lax.ppermute(array, ("zl", "zh"), [(place(z), place((z + step) % 8)) for z in range(8)])


def along_y(array, step):
    return lax.ppermute(array, "y", [(k, (k + step) % 4) for k in range(4)])


def swapped(array, axis):
    return lax.ppermute(array, axis, [(0, 1), (1, 0)])


def to_plane(array):
    copies = jnp.broadcast_to(array[None], (16, *array.shape))
    return lax.all_to_all(copies, PLANE, 0, 0, tiled=True)


def dot(a, b, dims):
    return lax.dot_general(a, b, (dims, ((), ())), preferred_element_type=F32)


def ring_gather(piece):
    half = piece.shape[0] // 2
    down, up = [piece], [piece]
    for _ in range(3):
        down.append(along_z(down[-1], 1))
        up.append(along_z(up[-1], -1))
    far = jnp.concatenate([along_z(down[3][:half], 1), along_z(up[3][half:], -1)])
    return jnp.concatenate([*down, far, up[3], up[2], up[1]])


def kernel(body, args, out_shape, scratch, copies, flops):
    hbm = pl.BlockSpec(memory_space=pl.ANY)
    return pl.pallas_call(
        body,
        in_specs=[pl.BlockSpec(memory_space=pltpu.SMEM)] + [hbm] * (len(args) - 1),
        out_specs=[hbm] * len(out_shape),
        out_shape=out_shape,
        scratch_shapes=[*scratch, pltpu.SemaphoreType.DMA((copies,))],
        compiler_params=pltpu.CompilerParams(vmem_limit_bytes=56 * 2**20),
        cost_estimate=pl.CostEstimate(
            flops=flops, transcendentals=0, bytes_accessed=flops // 512
        ),
        interpret=INTERPRET,
    )(*args)


class Copies:
    def __init__(self, sems):
        self.sems, self.used = sems, 0

    def start(self, source, target):
        copy = pltpu.make_async_copy(source, target, self.sems.at[self.used])
        self.used += 1
        copy.start()
        return copy


def wait(copies):
    for copy in copies:
        copy.wait()


def score_body(s, part, source, *refs, scale):
    first = len(source.shape) == 4
    if first:
        queries, passages, scores, stats, qv, pv, sv, tv, sems = refs
    else:
        passages, scores, stats, qv, pv, sv, tv, sems = refs
    _, quarter, wide = part.shape
    count, full = qv.shape
    rows, width = count // 4, full // 8
    copies = Copies(sems)
    ready = []
    for d in range(4):
        for h in range(2):
            piece = part.at[jnp.where((s[0] >= d) == (h == 0), d, d + 4)]
            at = pl.ds(d * quarter, quarter), pl.ds(h * wide, wide)
            ready.append(copies.start(piece, pv.at[at]))
    if first:
        came = []
        for x in range(4):
            for h in range(2):
                for k in range(4):
                    piece = source.at[x * 4 + (s[1] + 4 - k) % 4, h]
                    at = pl.ds(x * rows, rows), pl.ds((h * 4 + k) * width, width)
                    came.append(copies.start(piece, qv.at[at]))
    else:
        came = [copies.start(source, qv)]
    wait(ready)
    ends = [copies.start(pv, passages)]
    wait(came)
    if first:
        ends.append(copies.start(qv, queries))
    block = 2 * quarter
    wing = count // 2
    for j in range(2):
        found = []
        for k in range(2):
            at = slice(k * block, (k + 1) * block), slice(j * wing, (j + 1) * wing)
            values = dot(pv[at[0]], qv[at[1]], ((1,), (1,))) * scale
            sv[at] = values
            top = jnp.max(values, axis=0, keepdims=True)
            found.append((top, jnp.sum(jnp.exp(values - top), axis=0, keepdims=True)))
            spot = pl.ds(k * block, block), pl.ds(j * wing, wing)
            ends.append(copies.start(sv.at[spot], scores.at[spot]))
        top = jnp.maximum(found[0][0], found[1][0])
        total = found[0][1] * jnp.exp(found[0][0] - top) + found[1][1] * jnp.exp(found[1][0] - top)
        for k in range(2):
            tv[2 * j + k : 2 * j + k + 1] = top[:, k * rows : (k + 1) * rows]
            tv[4 + 2 * j + k : 5 + 2 * j + k] = total[:, k * rows : (k + 1) * rows]
    ends.append(copies.start(tv, stats))
    wait(ends)


def scored(scalars, part, source, count, full):
    half = 4 * part.shape[1]
    first = source.ndim == 4

    def body(*refs):
        score_body(*refs, scale=3.0 / math.sqrt(full))

    out = [SDS((count, full), BF16)] if first else []
    out += [SDS((half, full), BF16), SDS((half, count), F32), SDS((8, count // 4), F32)]
    scratch = [
        pltpu.VMEM((count, full), BF16),
        pltpu.VMEM((half, full), BF16),
        pltpu.VMEM((half, count), F32),
        pltpu.VMEM((8, count // 4), F32),
    ]
    return kernel(body, (scalars, part, source), out, scratch, 56, 2 * half * count * full)


def grad_body(s, s_own, s_other, log_total, targets, queries, p_own, p_other, *refs):
    d_own, d_other, terms, sv, gv, qv, pv, dv, tv, lv, iv, sems = refs
    half, count = s_own.shape
    full = qv.shape[1]
    block, quarter, rows, width = half // 2, half // 4, count // 4, full // 8
    copies = Copies(sems)
    small = [copies.start(log_total, lv), copies.start(targets, iv)]
    loads = []
    for b in range(4):
        source = (s_other, s_own)[b // 2].at[pl.ds(b % 2 * block, block)]
        loads.append(copies.start(source, sv.at[b]))
        if b == 0:
            query = copies.start(queries, qv)
    passage = [copies.start(p_other, pv.at[pl.ds(0, half)])]
    passage.append(copies.start(p_own, pv.at[pl.ds(half, half)]))
    wait(small)
    ends = []
    for b in range(4):
        loads[b].wait()
        for k in range(2):
            place = (1 - b // 2) * 4 + b % 2 * 2 + k
            at = slice(k * quarter, (k + 1) * quarter)
            ids = s[2 + place] + lax.broadcasted_iota(jnp.int32, (quarter, 1), 0)
            hit = (ids == iv[...]).astype(F32)
            value = (jnp.exp(sv[b, at] - lv[...]) - hit).astype(BF16)
            gv[b * block + k * quarter : b * block + (k + 1) * quarter] = value
        if b == 0:
            query.wait()
        dv[b] = dot(gv[b * block : (b + 1) * block], qv[...], ((1,), (0,)))
        target = (d_other, d_own)[b // 2].at[pl.ds(b % 2 * block, block)]
        ends.append(copies.start(dv.at[b], target))
    wait(passage)
    for x in range(4):
        at = slice(x * rows, (x + 1) * rows)
        tv[at] = dot(gv[:, at], pv[...], ((0,), (0,))).astype(BF16)
        for h in range(2):
            for k in range(4):
                piece = terms.at[x * 4 + (s[1] + 4 - k) % 4, h]
                spot = pl.ds(x * rows, rows), pl.ds((h * 4 + k) * width, width)
                ends.append(copies.start(tv.at[spot], piece))
    wait(ends)


def gradients(scalars, s_own, s_other, log_total, targets, queries, p_own, p_other):
    half, count = s_own.shape
    full = queries.shape[1]
    out = [
        SDS((half, full), F32),
        SDS((half, full), F32),
        SDS((16, 2, count // 4, full // 8), BF16),
    ]
    scratch = [
        pltpu.VMEM((4, half // 2, count), F32),
        pltpu.VMEM((2 * half, count), BF16),
        pltpu.VMEM((count, full), BF16),
        pltpu.VMEM((2 * half, full), BF16),
        pltpu.VMEM((4, half // 2, full), F32),
        pltpu.VMEM((count, full), BF16),
        pltpu.VMEM((1, count), F32),
        pltpu.VMEM((1, count), jnp.int32),
    ]
    args = (scalars, s_own, s_other, log_total, targets, queries, p_own, p_other)
    return kernel(grad_body, args, out, scratch, 48, 8 * half * count * full)


def combine_body(s, own, theirs, *refs):
    outs, (av, bv, ov, sems) = refs[:8], refs[8:]
    quarter, wide = outs[0].shape
    copies = Copies(sems)
    loads = []
    for d in range(4):
        at = pl.ds(d * quarter, quarter)
        loads.append((copies.start(own.at[at], av.at[at]), copies.start(theirs.at[at], bv.at[at])))
    ends = []
    for d in range(4):
        wait(loads[d])
        at = slice(d * quarter, (d + 1) * quarter)
        pair = (av[at] + bv[at]).astype(BF16)
        left, right = pair[:, :wide], pair[:, wide:]
        here = s[0] >= d
        ov[d] = jnp.where(here, left, right)
        ov[d + 4] = jnp.where(here, right, left)
        ends += [copies.start(ov.at[k], outs[k]) for k in (d, d + 4)]
    wait(ends)


def combined(scalars, own, theirs):
    half, full = own.shape
    quarter, wide = half // 4, full // 2
    scratch = [
        pltpu.VMEM((half, full), F32),
        pltpu.VMEM((half, full), F32),
        pltpu.VMEM((8, quarter, wide), BF16),
    ]
    out = [SDS((quarter, wide), BF16)] * 8
    return kernel(combine_body, (scalars, own, theirs), out, scratch, 16, 2**31)


def local(queries, passages, positive):
    return step(queries, passages, positive)


def step(queries, passages, positive):
    rows, width = queries.shape
    half, quarter = rows // 2, rows // 4
    full, count = 8 * width, 2 * rows
    x, y, c = (lax.axis_index(a) for a in ("x", "y", "c"))
    zl, zh = lax.axis_index("zl"), lax.axis_index("zh")

    kept = lax.dynamic_slice(queries, (zh * half, 0), (half, width))
    sent = lax.dynamic_slice(queries, ((1 - zh) * half, 0), (half, width))
    pieces = to_plane(jnp.stack([kept, swapped(sent, "zh")]))

    mine = [
        lax.dynamic_slice(passages, ((y + d) % 4 * quarter, 0), (quarter, width)) for d in range(4)
    ]
    passage_part = jnp.concatenate([mine[0]] + [along_y(mine[d], d) for d in (1, 2, 3)], axis=1)
    own = ring_gather(passage_part).reshape(8, quarter, 4 * width)
    other = swapped(own, "c")

    source_c = jnp.stack([c, 1 - c])
    group = (((zl - jnp.arange(4)) % 4) * 4 + x)[None, :] * 2 + source_c[:, None]
    first = (group * rows + y * quarter).reshape(8)
    scalars = jnp.concatenate([zl[None], y[None], first]).astype(jnp.int32)

    block_queries, p_own, s_own, t_own = scored(scalars, own, pieces, count, full)
    p_other, s_other, t_other = scored(scalars, other, block_queries, count, full)
    wanted = lax.dynamic_slice(positive, (zh * half,), (half,)).astype(F32)
    stats = to_plane(jnp.concatenate([t_own, t_other, wanted[None]]))
    peaks = jnp.concatenate([stats[:, :4], stats[:, 8:12]])
    totals = jnp.concatenate([stats[:, 4:8], stats[:, 12:16]])
    targets = stats[:, 16].reshape(4, 4, half)[:, 0].reshape(1, count).astype(jnp.int32)
    highest = jnp.max(peaks, axis=0)
    log_total = highest + jnp.log(jnp.sum(totals * jnp.exp(peaks - highest), axis=0))
    log_total = log_total.reshape(1, count)

    d_own, d_other, terms = gradients(
        scalars, s_own, s_other, log_total, targets, block_queries, p_own, p_other
    )
    theirs = swapped(d_other, "c")
    terms = lax.all_to_all(terms, PLANE, 0, 0, tiled=True)
    parts = combined(scalars, d_own, theirs)
    parts = [parts[0]] + [along_z(parts[d], -d) for d in (4, 3, 5, 2, 6, 1, 7)]

    total = parts[0].astype(F32)
    for part in parts[1:]:
        total += part.astype(F32)
    total = total.astype(BF16)
    slices = [total[:, k * width : (k + 1) * width] for k in range(4)]
    slices = [slices[0]] + [along_y(slices[k], -k) for k in (1, 2, 3)]
    grad_passages = jnp.zeros((rows, width), BF16)
    for k in range(4):
        grad_passages = lax.dynamic_update_slice(
            grad_passages, slices[k], ((y + k) % 4 * quarter, 0)
        )

    grad_queries = jnp.sum(terms.astype(F32), axis=0).astype(BF16)
    kept, received = grad_queries[0], swapped(grad_queries[1], "zh")
    grad_queries = jnp.where(
        zh == 0, jnp.concatenate([kept, received]), jnp.concatenate([received, kept])
    )
    return grad_queries, grad_passages


def solution(mesh):
    finer = Mesh(mesh.devices.reshape(4, 4, 2, 2, 4), ("zl", "x", "c", "zh", "y"))
    groups = ("zl", "x", "c")
    return jax.shard_map(
        step if INTERPRET else local,
        mesh=finer,
        in_specs=(P(groups, WIDTH), P(groups, WIDTH), P(groups)),
        out_specs=(P(groups, WIDTH), P(groups, WIDTH)),
        check_vma=False,
    )
```

```python
import functools
import math

import jax
import jax.numpy as jnp
from jax import lax
from jax.experimental import pallas as pl
from jax.experimental.pallas import tpu as pltpu
from jax.sharding import Mesh
from jax.sharding import PartitionSpec as P

WIDTH = ("zh", "y")
PLANE = ("x", "y")
F32, BF16 = jnp.float32, jnp.bfloat16
INTERPRET = False


def along_z(array, step):
    place = lambda z: (z % 4) * 2 + z // 4
    return lax.ppermute(array, ("zl", "zh"), [(place(z), place((z + step) % 8)) for z in range(8)])


def along(array, axis, step):
    return lax.ppermute(array, axis, [(k, (k + step) % 4) for k in range(4)])


def swapped(array, axis):
    return lax.ppermute(array, axis, [(0, 1), (1, 0)])


def to_plane(array):
    copies = jnp.broadcast_to(array[None], (16, *array.shape))
    return lax.all_to_all(copies, PLANE, 0, 0, tiled=True)


def dot(a, b, dims):
    return lax.dot_general(a, b, (dims, ((), ())), preferred_element_type=F32)


def ring_gather(piece):
    half = piece.shape[0] // 2
    down, up = [piece], [piece]
    for _ in range(3):
        down.append(along_z(down[-1], 1))
        up.append(along_z(up[-1], -1))
    far = jnp.concatenate([along_z(down[3][:half], 1), along_z(up[3][half:], -1)])
    return jnp.concatenate([piece, down[1], up[1], down[2], up[2], down[3], up[3], far])


SLOT = (0, 1, 3, 5, 7, 6, 4, 2)


def kernel(body, args, places, out_shape, scratch, copies, flops):
    hbm, vmem = pl.BlockSpec(memory_space=pl.ANY), pl.BlockSpec(memory_space=pltpu.VMEM)
    if not INTERPRET:
        args = [
            a
            if p == "s"
            else pltpu.with_memory_space_constraint(a, pltpu.VMEM if p == "v" else pltpu.HBM)
            for a, p in zip(args, places)
        ]
    spec_of = {"v": vmem, "h": hbm, "s": pl.BlockSpec(memory_space=pltpu.SMEM)}
    return pl.pallas_call(
        body,
        in_specs=[spec_of[p] for p in places],
        out_specs=[vmem if o.near else hbm for o in out_shape],
        out_shape=[o.placed() for o in out_shape],
        scratch_shapes=[*scratch, pltpu.SemaphoreType.DMA((copies,))],
        compiler_params=pltpu.CompilerParams(vmem_limit_bytes=26 * 2**20),
        cost_estimate=pl.CostEstimate(
            flops=flops, transcendentals=0, bytes_accessed=flops // 512
        ),
        interpret=INTERPRET,
    )(*args)


class Out:
    def __init__(self, near, shape, dtype):
        self.near, self.shape, self.dtype = near, shape, dtype

    def placed(self):
        if INTERPRET:
            return jax.ShapeDtypeStruct(self.shape, self.dtype)
        return (pltpu.VMEM if self.near else pltpu.HBM)(self.shape, self.dtype)


near = functools.partial(Out, True)
far = functools.partial(Out, False)


class Copies:
    def __init__(self, sems):
        self.sems, self.used = sems, 0

    def start(self, source, target):
        copy = pltpu.make_async_copy(source, target, self.sems.at[self.used])
        self.used += 1
        copy.start()
        return copy


def wait(copies):
    for copy in copies:
        copy.wait()


def score_body(s, part, source, *refs, scale):
    first = len(source.shape) == 4
    if first:
        queries, passages, scores, stats, sems = refs
    else:
        before, passages, scores, stats, sems = refs
        queries = source
    _, quarter, wide = part.shape
    count, full = queries.shape
    rows, width = count // 4, full // 8
    copies = Copies(sems)
    ready = []
    for d in range(4):
        for h in range(2):
            piece = part.at[jnp.where((s[0] >= d) == (h == 0), SLOT[d], SLOT[d + 4])]
            at = pl.ds(d * quarter, quarter), pl.ds(h * wide, wide)
            ready.append(copies.start(piece, passages.at[at]))
    if first:
        for x in range(4):
            for h in range(2):
                for k in range(4):
                    at = (h * 4 + k) * width
                    queries[x * rows : (x + 1) * rows, at : at + width] = source[
                        x * 4 + (s[1] + 4 - k) % 4, h
                    ]
    block = 2 * quarter
    wing = count // 2
    found = []
    for k in range(2):
        wait(ready[4 * k : 4 * k + 4])
        for j in range(2):
            at = slice(k * block, (k + 1) * block), slice(j * wing, (j + 1) * wing)
            values = dot(passages[at[0]], queries[at[1]], ((1,), (1,))) * scale
            scores[at] = values
            top = jnp.max(values, axis=0, keepdims=True)
            found.append((top, jnp.sum(jnp.exp(values - top), axis=0, keepdims=True)))
    for x in range(4):
        j, k = divmod(x, 2)
        at = slice(k * rows, (k + 1) * rows)
        seen = [(top[:, at], total[:, at]) for top, total in (found[j], found[2 + j])]
        if not first:
            seen.append((before[x : x + 1], before[4 + x : 5 + x]))
        top = seen[0][0]
        for other, _ in seen[1:]:
            top = jnp.maximum(top, other)
        stats[x : x + 1] = top
        stats[4 + x : 5 + x] = sum(total * jnp.exp(other - top) for other, total in seen)


def scored(scalars, part, source, before, count, full):
    half = 4 * part.shape[1]
    first = source.ndim == 4

    def body(*refs):
        score_body(*refs, scale=3.0 / math.sqrt(full))

    out = [near((count, full), BF16)] if first else []
    out += [
        near((half, full), BF16),
        near((half, count), F32),
        near((8, count // 4), F32),
    ]
    args = (scalars, part, source) if first else (scalars, part, source, before)
    return kernel(body, args, "shvv"[: len(args)], out, [], 8, 2 * half * count * full)


def grad_body(s, s_own, s_other, *refs):
    seen, refs = refs[:4], refs[4:]
    queries, p_own, p_other, d_own, d_other, terms, gv, dv, tv, sems = refs
    half, count = s_own.shape
    full = queries.shape[1]
    block, quarter, rows, width = half // 2, half // 4, count // 4, full // 8
    copies = Copies(sems)
    ends, logs, wanted = [], [], []
    for x in range(4):
        tops = [part[x : x + 1] for part in seen]
        top = functools.reduce(jnp.maximum, tops)
        total = sum(part[4 + x : 5 + x] * jnp.exp(high - top) for part, high in zip(seen, tops))
        logs.append(top + jnp.log(total))
        back = (s[10] + 4 - x) % 4
        wanted.append(sum(jnp.where(back == k, part[8:9], 0.0) for k, part in enumerate(seen)))
    log_total = jnp.concatenate(logs, axis=1)
    targets = jnp.concatenate(wanted, axis=1)
    for b in range(4):
        scores = (s_other, s_own)[b // 2]
        for k in range(2):
            place = (1 - b // 2) * 4 + b % 2 * 2 + k
            at = b % 2 * block + k * quarter
            ids = s[2 + place] + lax.broadcasted_iota(jnp.int32, (quarter, 1), 0)
            hit = (ids.astype(F32) == targets).astype(F32)
            value = (jnp.exp(scores[at : at + quarter] - log_total) - hit).astype(BF16)
            gv[b * block + k * quarter : b * block + (k + 1) * quarter] = value
        dv[b] = dot(gv[b * block : (b + 1) * block], queries[...], ((1,), (0,)))
        target = (d_other, d_own)[b // 2].at[pl.ds(b % 2 * block, block)]
        ends.append(copies.start(dv.at[b], target))
    for x in range(4):
        at = slice(x * rows, (x + 1) * rows)
        values = dot(gv[:half, at], p_other[...], ((0,), (0,)))
        values += dot(gv[half:, at], p_own[...], ((0,), (0,)))
        tv[at] = values.astype(BF16)
        for h in range(2):
            for k in range(4):
                piece = terms.at[x * 4 + (s[1] + 4 - k) % 4, h]
                spot = pl.ds(x * rows, rows), pl.ds((h * 4 + k) * width, width)
                ends.append(copies.start(tv.at[spot], piece))
    wait(ends)


def gradients(scalars, s_own, s_other, seen, queries, p_own, p_other):
    half, count = s_own.shape
    full = queries.shape[1]
    out = [
        far((half, full), F32),
        far((half, full), F32),
        far((16, 2, count // 4, full // 8), BF16),
    ]
    scratch = [
        pltpu.VMEM((2 * half, count), BF16),
        pltpu.VMEM((4, half // 2, full), F32),
        pltpu.VMEM((count, full), BF16),
    ]
    args = (scalars, s_own, s_other, *seen, queries, p_own, p_other)
    return kernel(grad_body, args, "s" + 9 * "v", out, scratch, 40, 8 * half * count * full)


def combine_body(s, own, theirs, *refs):
    outs, (av, bv, ov, sems) = refs[:8], refs[8:]
    quarter, wide = outs[0].shape
    copies = Copies(sems)
    loads = []
    for d in range(4):
        at = pl.ds(d * quarter, quarter)
        loads.append((copies.start(own.at[at], av.at[at]), copies.start(theirs.at[at], bv.at[at])))
    ends = []
    for d in range(4):
        wait(loads[d])
        at = slice(d * quarter, (d + 1) * quarter)
        pair = (av[at] + bv[at]).astype(BF16)
        left, right = pair[:, :wide], pair[:, wide:]
        here = s[0] >= d
        ov[d] = jnp.where(here, left, right)
        ov[d + 4] = jnp.where(here, right, left)
        ends += [copies.start(ov.at[k], outs[k]) for k in (d, d + 4)]
    wait(ends)


def combined(scalars, own, theirs):
    half, full = own.shape
    quarter, wide = half // 4, full // 2
    scratch = [
        pltpu.VMEM((half, full), F32),
        pltpu.VMEM((half, full), F32),
        pltpu.VMEM((8, quarter, wide), BF16),
    ]
    out = [far((quarter, wide), BF16)] * 8
    return kernel(combine_body, (scalars, own, theirs), "shh", out, scratch, 16, 2**31)


def local(queries, passages, positive):
    return step(queries, passages, positive)


def step(queries, passages, positive):
    rows, width = queries.shape
    half, quarter = rows // 2, rows // 4
    full, count = 8 * width, 2 * rows
    x, y, c = (lax.axis_index(a) for a in ("x", "y", "c"))
    zl, zh = lax.axis_index("zl"), lax.axis_index("zh")

    kept = lax.dynamic_slice(queries, (zh * half, 0), (half, width))
    sent = lax.dynamic_slice(queries, ((1 - zh) * half, 0), (half, width))
    copies = jnp.stack([kept, swapped(sent, "zh")])
    pieces = to_plane(copies)

    mine = [
        lax.dynamic_slice(passages, ((y + d) % 4 * quarter, 0), (quarter, width)) for d in range(4)
    ]
    crossed = [along(mine[d], "y", d) for d in (1, 2, 3)]
    passage_part = jnp.concatenate([mine[0], *crossed], axis=1)
    own = ring_gather(passage_part).reshape(8, quarter, 4 * width)
    other = swapped(own, "c")

    source_c = jnp.stack([c, 1 - c])
    group = (((zl - jnp.arange(4)) % 4) * 4 + x)[None, :] * 2 + source_c[:, None]
    first = (group * rows + y * quarter).reshape(8)
    scalars = jnp.concatenate([zl[None], y[None], first, x[None]]).astype(jnp.int32)

    block_queries, p_own, s_own, half_stats = scored(scalars, own, pieces, None, count, full)
    p_other, s_other, stats = scored(scalars, other, block_queries, half_stats, count, full)
    wanted = lax.dynamic_slice(positive, (zh * half,), (half,)).astype(F32)
    seen = [stats] + [along(stats, "y", d) for d in (1, 2, 3)]
    tops = functools.reduce(jnp.maximum, [part[:4] for part in seen])
    totals = sum(part[4:] * jnp.exp(part[:4] - tops) for part in seen)
    stats = jnp.concatenate([tops, totals, wanted[None]])
    seen = [stats] + [along(stats, "x", d) for d in (1, 2, 3)]

    d_own, d_other, terms = gradients(
        scalars, s_own, s_other, seen, block_queries, p_own, p_other
    )
    theirs = swapped(d_other, "c")
    terms = lax.all_to_all(terms, PLANE, 0, 0, tiled=True)
    parts = combined(scalars, d_own, theirs)
    parts = [parts[0]] + [along_z(parts[d], -d) for d in (4, 3, 5, 2, 6, 1, 7)]

    total = parts[0].astype(F32)
    for part in parts[1:]:
        total += part.astype(F32)
    total = total.astype(BF16)
    slices = [total[:, k * width : (k + 1) * width] for k in range(4)]
    slices = [slices[0]] + [along(slices[k], "y", -k) for k in (1, 2, 3)]
    grad_passages = jnp.zeros((rows, width), BF16)
    for k in range(4):
        grad_passages = lax.dynamic_update_slice(
            grad_passages, slices[k], ((y + k) % 4 * quarter, 0)
        )

    grad_queries = jnp.sum(terms.astype(F32), axis=0).astype(BF16)
    kept, received = grad_queries[0], swapped(grad_queries[1], "zh")
    grad_queries = jnp.where(
        zh == 0, jnp.concatenate([kept, received]), jnp.concatenate([received, kept])
    )
    return grad_queries, grad_passages


def solution(mesh):
    finer = Mesh(mesh.devices.reshape(4, 4, 2, 2, 4), ("zl", "x", "c", "zh", "y"))
    groups = ("zl", "x", "c")
    return jax.shard_map(
        step if INTERPRET else local,
        mesh=finer,
        in_specs=(P(groups, WIDTH), P(groups, WIDTH), P(groups)),
        out_specs=(P(groups, WIDTH), P(groups, WIDTH)),
        check_vma=False,
    )
```

```python
import functools
import math

import jax
import jax.numpy as jnp
from jax import lax
from jax.experimental import pallas as pl
from jax.experimental.pallas import tpu as pltpu
from jax.sharding import Mesh
from jax.sharding import PartitionSpec as P

WIDTH = ("zh", "y")
PLANE = ("x", "y")
F32, BF16 = jnp.float32, jnp.bfloat16
INTERPRET = False


def along_z(array, step):
    place = lambda z: (z % 4) * 2 + z // 4
    return lax.ppermute(array, ("zl", "zh"), [(place(z), place((z + step) % 8)) for z in range(8)])


def along(array, axis, step):
    return lax.ppermute(array, axis, [(k, (k + step) % 4) for k in range(4)])


def swapped(array, axis):
    return lax.ppermute(array, axis, [(0, 1), (1, 0)])


def to_plane(array):
    copies = jnp.broadcast_to(array[None], (16, *array.shape))
    return lax.all_to_all(copies, PLANE, 0, 0, tiled=True)


def dot(a, b, dims):
    return lax.dot_general(a, b, (dims, ((), ())), preferred_element_type=F32)


def ring_gather(piece):
    half = piece.shape[0] // 2
    down, up = [piece], [piece]
    for _ in range(3):
        down.append(along_z(down[-1], 1))
        up.append(along_z(up[-1], -1))
    far = jnp.concatenate([along_z(down[3][:half], 1), along_z(up[3][half:], -1)])
    return jnp.concatenate([piece, down[1], up[1], down[2], up[2], down[3], up[3], far])


SLOT = (0, 1, 3, 5, 7, 6, 4, 2)


def kernel(body, args, places, out_shape, scratch, copies, flops):
    hbm, vmem = pl.BlockSpec(memory_space=pl.ANY), pl.BlockSpec(memory_space=pltpu.VMEM)
    if not INTERPRET:
        args = [
            a
            if p == "s"
            else pltpu.with_memory_space_constraint(a, pltpu.VMEM if p == "v" else pltpu.HBM)
            for a, p in zip(args, places)
        ]
    spec_of = {"v": vmem, "h": hbm, "s": pl.BlockSpec(memory_space=pltpu.SMEM)}
    return pl.pallas_call(
        body,
        in_specs=[spec_of[p] for p in places],
        out_specs=[vmem if o.near else hbm for o in out_shape],
        out_shape=[o.placed() for o in out_shape],
        scratch_shapes=[*scratch, pltpu.SemaphoreType.DMA((copies,))],
        compiler_params=pltpu.CompilerParams(vmem_limit_bytes=26 * 2**20),
        cost_estimate=pl.CostEstimate(
            flops=flops, transcendentals=0, bytes_accessed=flops // 512
        ),
        interpret=INTERPRET,
    )(*args)


class Out:
    def __init__(self, near, shape, dtype):
        self.near, self.shape, self.dtype = near, shape, dtype

    def placed(self):
        if INTERPRET:
            return jax.ShapeDtypeStruct(self.shape, self.dtype)
        return (pltpu.VMEM if self.near else pltpu.HBM)(self.shape, self.dtype)


near = functools.partial(Out, True)
far = functools.partial(Out, False)


class Copies:
    def __init__(self, sems):
        self.sems, self.used = sems, 0

    def start(self, source, target):
        copy = pltpu.make_async_copy(source, target, self.sems.at[self.used])
        self.used += 1
        copy.start()
        return copy


def wait(copies):
    for copy in copies:
        copy.wait()


def score_body(s, part, source, *refs, scale):
    first = len(source.shape) == 4
    if first:
        queries, passages, scores, stats, sems = refs
    else:
        before, passages, scores, stats, sems = refs
        queries = source
    _, quarter, wide = part.shape
    count, full = queries.shape
    rows, width = count // 4, full // 8
    copies = Copies(sems)
    ready = []
    for d in range(4):
        for h in range(2):
            piece = part.at[jnp.where((s[0] >= d) == (h == 0), SLOT[d], SLOT[d + 4])]
            at = pl.ds(d * quarter, quarter), pl.ds(h * wide, wide)
            ready.append(copies.start(piece, passages.at[at]))
    if first:
        for x in range(4):
            for h in range(2):
                for k in range(4):
                    at = (h * 4 + k) * width
                    queries[x * rows : (x + 1) * rows, at : at + width] = source[
                        x * 4 + (s[1] + 4 - k) % 4, h
                    ]
    block = 2 * quarter
    wing = count // 2
    wait(ready)

    def chunk(k, found):
        fresh = []
        rows_at = pl.ds(pl.multiple_of(k * block, block), block)
        for j in range(2):
            at = slice(j * wing, (j + 1) * wing)
            values = dot(passages[rows_at], queries[at], ((1,), (1,))) * scale
            scores[rows_at, at] = values
            high, total = found[j]
            top = jnp.maximum(high, jnp.max(values, axis=0, keepdims=True))
            total = total * jnp.exp(high - top)
            fresh.append((top, total + jnp.sum(jnp.exp(values - top), axis=0, keepdims=True)))
        return tuple(fresh)

    def wide_row(k, j):
        return jnp.concatenate([before[4 * k + 2 * j + n : 4 * k + 2 * j + n + 1] for n in (0, 1)], 1)

    if first:
        low, none = jnp.full((1, wing), -jnp.inf, F32), jnp.zeros((1, wing), F32)
        start = ((low, none), (low, none))
    else:
        start = tuple((wide_row(0, j), wide_row(1, j)) for j in range(2))
    found = lax.fori_loop(0, 2, chunk, start)
    for x in range(4):
        j, k = divmod(x, 2)
        at = slice(k * rows, (k + 1) * rows)
        stats[x : x + 1] = found[j][0][:, at]
        stats[4 + x : 5 + x] = found[j][1][:, at]


def scored(scalars, part, source, before, count, full):
    half = 4 * part.shape[1]
    first = source.ndim == 4

    def body(*refs):
        score_body(*refs, scale=3.0 / math.sqrt(full))

    out = [near((count, full), BF16)] if first else []
    out += [
        near((half, full), BF16),
        near((half, count), F32),
        near((8, count // 4), F32),
    ]
    args = (scalars, part, source) if first else (scalars, part, source, before)
    return kernel(body, args, "shvv"[: len(args)], out, [], 8, 2 * half * count * full)


def grad_body(s, s_own, s_other, *refs):
    seen, refs = refs[:4], refs[4:]
    queries, p_own, p_other, d_own, d_other, terms, gv, bv, dv, tv, sems = refs
    half, count = s_own.shape
    full = queries.shape[1]
    block, quarter, rows, width = half // 2, half // 4, count // 4, full // 8
    logs, wanted = [], []
    for x in range(4):
        tops = [part[x : x + 1] for part in seen]
        top = functools.reduce(jnp.maximum, tops)
        total = sum(part[4 + x : 5 + x] * jnp.exp(high - top) for part, high in zip(seen, tops))
        logs.append(top + jnp.log(total))
        back = (s[10] + 4 - x) % 4
        wanted.append(sum(jnp.where(back == k, part[8:9], 0.0) for k, part in enumerate(seen)))
    log_total = jnp.concatenate(logs, axis=1)
    targets = jnp.concatenate(wanted, axis=1)

    def sent(source, b):
        target = (d_other, d_own)[source].at[pl.ds(b * block, block)]
        return pltpu.make_async_copy(dv.at[2 * source + b], target, sems.at[2 * source + b])

    def leaving(x, h, k):
        piece = terms.at[x * 4 + (s[1] + 4 - k) % 4, h]
        spot = tv.at[x, :, pl.ds((h * 4 + k) * width, width)]
        return pltpu.make_async_copy(spot, piece, sems.at[4 + 8 * x + 4 * h + k])

    for source, scores in enumerate((s_other, s_own)):

        def one(b, _):
            for k in range(2):
                base = s[2 + (1 - source) * 4 + 2 * b + k]
                ids = base + lax.broadcasted_iota(jnp.int32, (quarter, 1), 0)
                hit = (ids.astype(F32) == targets).astype(F32)
                at = pl.ds(pl.multiple_of(b * block + k * quarter, quarter), quarter)
                value = (jnp.exp(scores[at] - log_total) - hit).astype(BF16)
                bv[k * quarter : (k + 1) * quarter] = value
                at = source * half + b * block + k * quarter
                at = pl.ds(pl.multiple_of(at, quarter), quarter)
                for x in range(4):
                    gv[x, at] = value[:, x * rows : (x + 1) * rows]
            dv[2 * source + b] = dot(bv[...], queries[...], ((1,), (0,)))
            sent(source, b).start()
            return 0

        lax.fori_loop(0, 2, one, 0, unroll=True)

    def another(x, _):
        values = dot(gv[x, :half], p_other[...], ((0,), (0,)))
        values += dot(gv[x, half:], p_own[...], ((0,), (0,)))
        tv[x] = values.astype(BF16)
        for h in range(2):
            for k in range(4):
                leaving(x, h, k).start()
        return 0

    lax.fori_loop(0, 4, another, 0)
    for source in range(2):
        for b in range(2):
            sent(source, b).wait()
    for x in range(4):
        for h in range(2):
            for k in range(4):
                leaving(x, h, k).wait()


def gradients(scalars, s_own, s_other, seen, queries, p_own, p_other):
    half, count = s_own.shape
    full = queries.shape[1]
    out = [
        far((half, full), F32),
        far((half, full), F32),
        far((16, 2, count // 4, full // 8), BF16),
    ]
    scratch = [
        pltpu.VMEM((4, 2 * half, count // 4), BF16),
        pltpu.VMEM((half // 2, count), BF16),
        pltpu.VMEM((4, half // 2, full), F32),
        pltpu.VMEM((4, count // 4, full), BF16),
    ]
    args = (scalars, s_own, s_other, *seen, queries, p_own, p_other)
    return kernel(grad_body, args, "s" + 9 * "v", out, scratch, 40, 8 * half * count * full)


def combine_body(s, own, theirs, *refs):
    outs, (av, bv, fv, ov, sems) = refs[:9], refs[9:]
    quarter, wide = outs[0].shape
    half = quarter // 2
    copies = Copies(sems)
    order = (3, 0, 2, 1)
    loads = {}
    for d in order:
        at = pl.ds(d * quarter, quarter)
        loads[d] = (
            copies.start(own.at[at], av.at[at]),
            copies.start(theirs.at[at], bv.at[at]),
        )
    ends = []
    for d in order:
        wait(loads[d])
        at = slice(d * quarter, (d + 1) * quarter)
        pair = av[at] + bv[at]
        left, right = pair[:, :wide], pair[:, wide:]
        here = s[0] >= d
        for k, value in ((d, jnp.where(here, left, right)), (d + 4, jnp.where(here, right, left))):
            if k in (0, 1, 7):
                place = (0, 1, 7).index(k)
                fv[place] = value
                ends.append(copies.start(fv.at[place], outs[place]))
                continue
            ov[k - 2] = value.astype(BF16)
            if k == 4:
                ends.append(copies.start(ov.at[2, pl.ds(0, half)], outs[7]))
                ends.append(copies.start(ov.at[2, pl.ds(half, half)], outs[8]))
            else:
                ends.append(copies.start(ov.at[k - 2], outs[3 + (2, 3, 5, 6).index(k)]))
    wait(ends)


def combined(scalars, own, theirs):
    rows, full = own.shape
    quarter, wide = rows // 4, full // 2
    scratch = [
        pltpu.VMEM((rows, full), F32),
        pltpu.VMEM((rows, full), F32),
        pltpu.VMEM((3, quarter, wide), F32),
        pltpu.VMEM((5, quarter, wide), BF16),
    ]
    out = [far((quarter, wide), F32)] * 3 + [far((quarter, wide), BF16)] * 4
    out += [far((quarter // 2, wide), BF16)] * 2
    return kernel(combine_body, (scalars, own, theirs), "shh", out, scratch, 17, 2**31)


def local(queries, passages, positive):
    return step(queries, passages, positive)


def step(queries, passages, positive):
    rows, width = queries.shape
    half, quarter = rows // 2, rows // 4
    full, count = 8 * width, 2 * rows
    x, y, c = (lax.axis_index(a) for a in ("x", "y", "c"))
    zl, zh = lax.axis_index("zl"), lax.axis_index("zh")

    kept = lax.dynamic_slice(queries, (zh * half, 0), (half, width))
    sent = lax.dynamic_slice(queries, ((1 - zh) * half, 0), (half, width))
    copies = jnp.stack([kept, swapped(sent, "zh")])
    pieces = to_plane(copies)

    mine = [
        lax.dynamic_slice(passages, ((y + d) % 4 * quarter, 0), (quarter, width)) for d in range(4)
    ]
    crossed = [along(mine[d], "y", d) for d in (1, 2, 3)]
    passage_part = jnp.concatenate([mine[0], *crossed], axis=1)
    own = ring_gather(passage_part).reshape(8, quarter, 4 * width)
    other = swapped(own, "c")

    source_c = jnp.stack([c, 1 - c])
    group = (((zl - jnp.arange(4)) % 4) * 4 + x)[None, :] * 2 + source_c[:, None]
    first = (group * rows + y * quarter).reshape(8)
    scalars = jnp.concatenate([zl[None], y[None], first, x[None]]).astype(jnp.int32)

    block_queries, p_own, s_own, half_stats = scored(scalars, own, pieces, None, count, full)
    p_other, s_other, stats = scored(scalars, other, block_queries, half_stats, count, full)
    wanted = lax.dynamic_slice(positive, (zh * half,), (half,)).astype(F32)
    seen = [stats] + [along(stats, "y", d) for d in (1, 2, 3)]
    tops = functools.reduce(jnp.maximum, [part[:4] for part in seen])
    totals = sum(part[4:] * jnp.exp(part[:4] - tops) for part in seen)
    stats = jnp.concatenate([tops, totals, wanted[None]])
    seen = [stats] + [along(stats, "x", d) for d in (1, 2, 3)]

    d_own, d_other, terms = gradients(
        scalars, s_own, s_other, seen, block_queries, p_own, p_other
    )
    theirs = swapped(d_other, "c")
    terms = lax.all_to_all(terms, PLANE, 0, 0, tiled=True)
    mine, down, up, d2, d3, d5, d6, low, high = combined(scalars, d_own, theirs)
    low, high = along_z(low, -3), along_z(high, 3)
    d3, d5 = along_z(d3, -2), along_z(d5, 2)
    d2, d6 = along_z(d2, -2), along_z(d6, 2)
    rest, rest_up = ((0, quarter // 2), (0, 0)), ((quarter // 2, 0), (0, 0))
    down = (down + d3.astype(F32) + jnp.pad(low.astype(F32), rest)).astype(BF16)
    up = (up + d5.astype(F32) + jnp.pad(high.astype(F32), rest_up)).astype(BF16)
    down, up = along_z(down, -1), along_z(up, 1)
    total = mine
    for part in (d2, d6, down, up):
        total += part.astype(F32)
    total = total.astype(BF16)
    slices = [total[:, k * width : (k + 1) * width] for k in range(4)]
    slices = [slices[0]] + [along(slices[k], "y", -k) for k in (1, 2, 3)]
    grad_passages = jnp.concatenate(
        [lax.select_n((q + 4 - y) % 4, *slices) for q in range(4)]
    )

    grad_queries = jnp.sum(terms.astype(F32), axis=0).astype(BF16)
    kept, received = grad_queries[0], swapped(grad_queries[1], "zh")
    grad_queries = jnp.where(
        zh == 0, jnp.concatenate([kept, received]), jnp.concatenate([received, kept])
    )
    return grad_queries, grad_passages


def solution(mesh):
    finer = Mesh(mesh.devices.reshape(4, 4, 2, 2, 4), ("zl", "x", "c", "zh", "y"))
    groups = ("zl", "x", "c")
    return jax.shard_map(
        step if INTERPRET else local,
        mesh=finer,
        in_specs=(P(groups, WIDTH), P(groups, WIDTH), P(groups)),
        out_specs=(P(groups, WIDTH), P(groups, WIDTH)),
        check_vma=False,
    )
```

```python
import functools
import math

import jax
import jax.numpy as jnp
from jax import lax
from jax.experimental import pallas as pl
from jax.experimental.pallas import tpu as pltpu
from jax.sharding import Mesh
from jax.sharding import PartitionSpec as P

WIDTH = ("zh", "y")
PLANE = ("x", "y")
F32, BF16 = jnp.float32, jnp.bfloat16
INTERPRET = False


def along_z(array, step):
    place = lambda z: (z % 4) * 2 + z // 4
    return lax.ppermute(array, ("zl", "zh"), [(place(z), place((z + step) % 8)) for z in range(8)])


def along(array, axis, step):
    return lax.ppermute(array, axis, [(k, (k + step) % 4) for k in range(4)])


def swapped(array, axis):
    return lax.ppermute(array, axis, [(0, 1), (1, 0)])


def to_plane(array):
    copies = jnp.broadcast_to(array[None], (16, *array.shape))
    return lax.all_to_all(copies, PLANE, 0, 0, tiled=True)


def dot(a, b, dims):
    return lax.dot_general(a, b, (dims, ((), ())), preferred_element_type=F32)


def ring_gather(piece):
    half = piece.shape[0] // 2
    down, up = [piece], [piece]
    for _ in range(3):
        down.append(along_z(down[-1], 1))
        up.append(along_z(up[-1], -1))
    far = jnp.concatenate([along_z(down[3][:half], 1), along_z(up[3][half:], -1)])
    return jnp.concatenate([piece, down[1], up[1], down[2], up[2], down[3], up[3], far])


SLOT = (0, 1, 3, 5, 7, 6, 4, 2)


def kernel(body, args, places, out_shape, scratch, copies, flops):
    hbm, vmem = pl.BlockSpec(memory_space=pl.ANY), pl.BlockSpec(memory_space=pltpu.VMEM)
    if not INTERPRET:
        args = [
            a
            if p == "s"
            else pltpu.with_memory_space_constraint(a, pltpu.VMEM if p == "v" else pltpu.HBM)
            for a, p in zip(args, places)
        ]
    spec_of = {"v": vmem, "h": hbm, "s": pl.BlockSpec(memory_space=pltpu.SMEM)}
    return pl.pallas_call(
        body,
        in_specs=[spec_of[p] for p in places],
        out_specs=[vmem if o.near else hbm for o in out_shape],
        out_shape=[o.placed() for o in out_shape],
        scratch_shapes=[*scratch, pltpu.SemaphoreType.DMA((copies,))],
        compiler_params=pltpu.CompilerParams(vmem_limit_bytes=26 * 2**20),
        cost_estimate=pl.CostEstimate(
            flops=flops, transcendentals=0, bytes_accessed=flops // 512
        ),
        interpret=INTERPRET,
    )(*args)


class Out:
    def __init__(self, near, shape, dtype):
        self.near, self.shape, self.dtype = near, shape, dtype

    def placed(self):
        if INTERPRET:
            return jax.ShapeDtypeStruct(self.shape, self.dtype)
        return (pltpu.VMEM if self.near else pltpu.HBM)(self.shape, self.dtype)


near = functools.partial(Out, True)
far = functools.partial(Out, False)


class Copies:
    def __init__(self, sems):
        self.sems, self.used = sems, 0

    def start(self, source, target):
        copy = pltpu.make_async_copy(source, target, self.sems.at[self.used])
        self.used += 1
        copy.start()
        return copy


def wait(copies):
    for copy in copies:
        copy.wait()


def score_body(s, own, other, pieces, queries, passages, scores, stats, sems, *, scale):
    _, quarter, wide = own.shape
    count, full = queries.shape
    rows, width = count // 4, full // 8
    copies = Copies(sems)
    ready = []
    for c, part in enumerate((own, other)):
        for d in range(4):
            for h in range(2):
                piece = part.at[jnp.where((s[0] >= d) == (h == 0), SLOT[d], SLOT[d + 4])]
                at = pl.ds((4 * c + d) * quarter, quarter), pl.ds(h * wide, wide)
                ready.append(copies.start(piece, passages.at[at]))
    for x in range(4):
        for h in range(2):
            for k in range(4):
                at = (h * 4 + k) * width
                queries[x * rows : (x + 1) * rows, at : at + width] = pieces[
                    x * 4 + (s[1] + 4 - k) % 4, h
                ]
    block = 2 * quarter
    wing = count // 2
    low, none = jnp.full((1, wing), -jnp.inf, F32), jnp.zeros((1, wing), F32)
    wait(ready)

    def chunk(k, found):
        fresh = []
        rows_at = pl.ds(pl.multiple_of(k * block, block), block)
        for j in range(2):
            at = slice(j * wing, (j + 1) * wing)
            values = dot(passages[rows_at], queries[at], ((1,), (1,))) * scale
            scores[rows_at, at] = values
            high, total = found[j]
            top = jnp.maximum(high, jnp.max(values, axis=0, keepdims=True))
            total = total * jnp.exp(high - top)
            fresh.append((top, total + jnp.sum(jnp.exp(values - top), axis=0, keepdims=True)))
        return tuple(fresh)

    found = lax.fori_loop(0, 4, chunk, ((low, none), (low, none)), unroll=UNROLL[0])
    for x in range(4):
        j, k = divmod(x, 2)
        at = slice(k * rows, (k + 1) * rows)
        stats[x : x + 1] = found[j][0][:, at]
        stats[4 + x : 5 + x] = found[j][1][:, at]


UNROLL = (1, True, 2)


def scored(scalars, own, other, pieces):
    _, _, rows, width = pieces.shape
    count, full, half = 4 * rows, 8 * width, 4 * own.shape[1]

    def body(*refs):
        score_body(*refs, scale=3.0 / math.sqrt(full))

    out = [near((count, full), BF16)]
    out += [near((2 * half, full), BF16), near((2 * half, count), F32), near((8, rows), F32)]
    return kernel(
        body, (scalars, own, other, pieces), "shhv", out, [], 16, 4 * half * count * full
    )


def grad_body(s, scores, *refs):
    seen, refs = refs[:4], refs[4:]
    queries, passages, d_own, d_other, terms, gv, bv, dv, tv, sems = refs
    half, count = scores.shape[0] // 2, scores.shape[1]
    full = queries.shape[1]
    block, quarter, rows, width = half // 2, half // 4, count // 4, full // 8
    logs, wanted = [], []
    for x in range(4):
        tops = [part[x : x + 1] for part in seen]
        top = functools.reduce(jnp.maximum, tops)
        total = sum(part[4 + x : 5 + x] * jnp.exp(high - top) for part, high in zip(seen, tops))
        logs.append(top + jnp.log(total))
        back = (s[10] + 4 - x) % 4
        wanted.append(sum(jnp.where(back == k, part[8:9], 0.0) for k, part in enumerate(seen)))
    log_total = jnp.concatenate(logs, axis=1)
    targets = jnp.concatenate(wanted, axis=1)

    def sent(source, b):
        target = (d_other, d_own)[source].at[pl.ds(b * block, block)]
        return pltpu.make_async_copy(dv.at[2 * source + b], target, sems.at[2 * source + b])

    def leaving(x, h, k):
        piece = terms.at[x * 4 + (s[1] + 4 - k) % 4, h]
        spot = tv.at[x, :, pl.ds((h * 4 + k) * width, width)]
        return pltpu.make_async_copy(spot, piece, sems.at[4 + 8 * x + 4 * h + k])

    for source in range(2):

        def one(b, _, source=source):
            for k in range(2):
                base = (1 - source) * half + b * block + k * quarter
                place = (1 - source) * 4 + 2 * b + k
                ids = s[2 + place] + lax.broadcasted_iota(jnp.int32, (quarter, 1), 0)
                hit = (ids.astype(F32) == targets).astype(F32)
                at = pl.ds(pl.multiple_of(base, quarter), quarter)
                value = (jnp.exp(scores[at] - log_total) - hit).astype(BF16)
                bv[k * quarter : (k + 1) * quarter] = value
                for x in range(4):
                    gv[x, at] = value[:, x * rows : (x + 1) * rows]
            dv[2 * source + b] = dot(bv[...], queries[...], ((1,), (0,)))
            sent(source, b).start()
            return 0

        lax.fori_loop(0, 2, one, 0, unroll=UNROLL[1])

    def another(x, _):
        tv[x] = dot(gv[x], passages[...], ((0,), (0,))).astype(BF16)
        for h in range(2):
            for k in range(4):
                leaving(x, h, k).start()
        return 0

    lax.fori_loop(0, 4, another, 0, unroll=UNROLL[2])
    for source in range(2):
        for b in range(2):
            sent(source, b).wait()
    for x in range(4):
        for h in range(2):
            for k in range(4):
                leaving(x, h, k).wait()


def gradients(scalars, scores, seen, queries, passages):
    half, count = scores.shape[0] // 2, scores.shape[1]
    full = queries.shape[1]
    out = [
        far((half, full), F32),
        far((half, full), F32),
        far((16, 2, count // 4, full // 8), BF16),
    ]
    scratch = [
        pltpu.VMEM((4, 2 * half, count // 4), BF16),
        pltpu.VMEM((half // 2, count), BF16),
        pltpu.VMEM((4, half // 2, full), F32),
        pltpu.VMEM((4, count // 4, full), BF16),
    ]
    args = (scalars, scores, *seen, queries, passages)
    return kernel(grad_body, args, "s" + 7 * "v", out, scratch, 40, 8 * half * count * full)


def combine_body(s, own, theirs, *refs):
    outs, (av, bv, fv, ov, sems) = refs[:9], refs[9:]
    quarter, wide = outs[0].shape
    half = quarter // 2
    copies = Copies(sems)
    order = (3, 0, 2, 1)
    loads = {}
    for d in order:
        at = pl.ds(d * quarter, quarter)
        loads[d] = (
            copies.start(own.at[at], av.at[at]),
            copies.start(theirs.at[at], bv.at[at]),
        )
    ends = []
    for d in order:
        wait(loads[d])
        at = slice(d * quarter, (d + 1) * quarter)
        pair = av[at] + bv[at]
        left, right = pair[:, :wide], pair[:, wide:]
        here = s[0] >= d
        for k, value in ((d, jnp.where(here, left, right)), (d + 4, jnp.where(here, right, left))):
            if k in (0, 1, 7):
                place = (0, 1, 7).index(k)
                fv[place] = value
                ends.append(copies.start(fv.at[place], outs[place]))
                continue
            ov[k - 2] = value.astype(BF16)
            if k == 4:
                ends.append(copies.start(ov.at[2, pl.ds(0, half)], outs[7]))
                ends.append(copies.start(ov.at[2, pl.ds(half, half)], outs[8]))
            else:
                ends.append(copies.start(ov.at[k - 2], outs[3 + (2, 3, 5, 6).index(k)]))
    wait(ends)


def combined(scalars, own, theirs):
    rows, full = own.shape
    quarter, wide = rows // 4, full // 2
    scratch = [
        pltpu.VMEM((rows, full), F32),
        pltpu.VMEM((rows, full), F32),
        pltpu.VMEM((3, quarter, wide), F32),
        pltpu.VMEM((5, quarter, wide), BF16),
    ]
    out = [far((quarter, wide), F32)] * 3 + [far((quarter, wide), BF16)] * 4
    out += [far((quarter // 2, wide), BF16)] * 2
    return kernel(combine_body, (scalars, own, theirs), "shh", out, scratch, 17, 2**31)


def local(queries, passages, positive):
    return step(queries, passages, positive)


def step(queries, passages, positive):
    rows, width = queries.shape
    half, quarter = rows // 2, rows // 4
    x, y, c = (lax.axis_index(a) for a in ("x", "y", "c"))
    zl, zh = lax.axis_index("zl"), lax.axis_index("zh")

    kept = lax.dynamic_slice(queries, (zh * half, 0), (half, width))
    sent = lax.dynamic_slice(queries, ((1 - zh) * half, 0), (half, width))
    copies = jnp.stack([kept, swapped(sent, "zh")])
    pieces = to_plane(copies)

    mine = [
        lax.dynamic_slice(passages, ((y + d) % 4 * quarter, 0), (quarter, width)) for d in range(4)
    ]
    crossed = [along(mine[d], "y", d) for d in (1, 2, 3)]
    passage_part = jnp.concatenate([mine[0], *crossed], axis=1)
    own = ring_gather(passage_part).reshape(8, quarter, 4 * width)
    other = swapped(own, "c")

    source_c = jnp.stack([c, 1 - c])
    group = (((zl - jnp.arange(4)) % 4) * 4 + x)[None, :] * 2 + source_c[:, None]
    first = (group * rows + y * quarter).reshape(8)
    scalars = jnp.concatenate([zl[None], y[None], first, x[None]]).astype(jnp.int32)

    block_queries, block_passages, scores, stats = scored(scalars, own, other, pieces)
    wanted = lax.dynamic_slice(positive, (zh * half,), (half,)).astype(F32)
    seen = [stats] + [along(stats, "y", d) for d in (1, 2, 3)]
    tops = functools.reduce(jnp.maximum, [part[:4] for part in seen])
    totals = sum(part[4:] * jnp.exp(part[:4] - tops) for part in seen)
    stats = jnp.concatenate([tops, totals, wanted[None]])
    seen = [stats] + [along(stats, "x", d) for d in (1, 2, 3)]

    d_own, d_other, terms = gradients(scalars, scores, seen, block_queries, block_passages)
    theirs = swapped(d_other, "c")
    terms = lax.all_to_all(terms, PLANE, 0, 0, tiled=True)
    mine, down, up, d2, d3, d5, d6, low, high = combined(scalars, d_own, theirs)
    low, high = along_z(low, -3), along_z(high, 3)
    d3, d5 = along_z(d3, -2), along_z(d5, 2)
    d2, d6 = along_z(d2, -2), along_z(d6, 2)
    rest, rest_up = ((0, quarter // 2), (0, 0)), ((quarter // 2, 0), (0, 0))
    down = (down + d3.astype(F32) + jnp.pad(low.astype(F32), rest)).astype(BF16)
    up = (up + d5.astype(F32) + jnp.pad(high.astype(F32), rest_up)).astype(BF16)
    down, up = along_z(down, -1), along_z(up, 1)
    total = mine
    for part in (d2, d6, down, up):
        total += part.astype(F32)
    total = total.astype(BF16)
    slices = [total[:, k * width : (k + 1) * width] for k in range(4)]
    slices = [slices[0]] + [along(slices[k], "y", -k) for k in (1, 2, 3)]
    grad_passages = jnp.concatenate(
        [lax.select_n((q + 4 - y) % 4, *slices) for q in range(4)]
    )

    grad_queries = jnp.sum(terms.astype(F32), axis=0).astype(BF16)
    kept, received = grad_queries[0], swapped(grad_queries[1], "zh")
    grad_queries = jnp.where(
        zh == 0, jnp.concatenate([kept, received]), jnp.concatenate([received, kept])
    )
    return grad_queries, grad_passages


def solution(mesh):
    finer = Mesh(mesh.devices.reshape(4, 4, 2, 2, 4), ("zl", "x", "c", "zh", "y"))
    groups = ("zl", "x", "c")
    return jax.shard_map(
        step if INTERPRET else local,
        mesh=finer,
        in_specs=(P(groups, WIDTH), P(groups, WIDTH), P(groups)),
        out_specs=(P(groups, WIDTH), P(groups, WIDTH)),
        check_vma=False,
    )
```

```python
import functools
import math

import jax
import jax.numpy as jnp
from jax import lax
from jax.experimental import pallas as pl
from jax.experimental.pallas import tpu as pltpu
from jax.sharding import Mesh
from jax.sharding import PartitionSpec as P

WIDTH = ("zh", "y")
PLANE = ("x", "y")
F32, BF16 = jnp.float32, jnp.bfloat16
INTERPRET = False


def along_z(array, step):
    place = lambda z: (z % 4) * 2 + z // 4
    return lax.ppermute(array, ("zl", "zh"), [(place(z), place((z + step) % 8)) for z in range(8)])


def along(array, axis, step):
    return lax.ppermute(array, axis, [(k, (k + step) % 4) for k in range(4)])


def swapped(array, axis):
    return lax.ppermute(array, axis, [(0, 1), (1, 0)])


def dot(a, b, dims):
    return lax.dot_general(a, b, (dims, ((), ())), preferred_element_type=F32)


def ring_gather(piece):
    half = piece.shape[0] // 2
    down, up = [piece], [piece]
    for _ in range(3):
        down.append(along_z(down[-1], 1))
        up.append(along_z(up[-1], -1))
    far = jnp.concatenate([along_z(down[3][:half], 1), along_z(up[3][half:], -1)])
    return jnp.concatenate([piece, down[1], up[1], down[2], up[2], down[3], up[3], far])


SLOT = (0, 1, 3, 5, 7, 6, 4, 2)


def kernel(body, args, places, out_shape, scratch, copies, flops, aliases=None):
    hbm, vmem = pl.BlockSpec(memory_space=pl.ANY), pl.BlockSpec(memory_space=pltpu.VMEM)
    if not INTERPRET:
        args = [
            a
            if p == "s"
            else pltpu.with_memory_space_constraint(a, pltpu.VMEM if p == "v" else pltpu.HBM)
            for a, p in zip(args, places)
        ]
    spec_of = {"v": vmem, "h": hbm, "s": pl.BlockSpec(memory_space=pltpu.SMEM)}
    return pl.pallas_call(
        body,
        in_specs=[spec_of[p] for p in places],
        out_specs=[vmem if o.near else hbm for o in out_shape],
        out_shape=[o.placed() for o in out_shape],
        scratch_shapes=[*scratch, pltpu.SemaphoreType.DMA((copies,))],
        compiler_params=pltpu.CompilerParams(vmem_limit_bytes=26 * 2**20),
        cost_estimate=pl.CostEstimate(
            flops=flops, transcendentals=0, bytes_accessed=flops // 512
        ),
        input_output_aliases=aliases or {},
        interpret=INTERPRET,
    )(*args)


class Out:
    def __init__(self, near, shape, dtype):
        self.near, self.shape, self.dtype = near, shape, dtype

    def placed(self):
        if INTERPRET:
            return jax.ShapeDtypeStruct(self.shape, self.dtype)
        return (pltpu.VMEM if self.near else pltpu.HBM)(self.shape, self.dtype)


near = functools.partial(Out, True)
far = functools.partial(Out, False)


class Copies:
    def __init__(self, sems):
        self.sems, self.used = sems, 0

    def start(self, source, target):
        copy = pltpu.make_async_copy(source, target, self.sems.at[self.used])
        self.used += 1
        copy.start()
        return copy


def wait(copies):
    for copy in copies:
        copy.wait()


def copies_of(array, place, before=None):
    def body(source, *refs):
        *_, out, sems = refs
        copies = Copies(sems)
        wait([copies.start(source, out.at[n, place]) for n in range(16)])

    args = (array,) if before is None else (array, before)
    out = [far((16, 2, *array.shape), array.dtype)]
    aliases = None if before is None else {1: 0}
    return kernel(body, args, "vh"[: len(args)], out, [], 16, 2**24, aliases)[0]


def score_body(s, own, other, pieces, queries, passages, scores, stats, sems, *, scale):
    _, quarter, wide = own.shape
    count, full = queries.shape
    rows, width = count // 4, full // 8
    copies = Copies(sems)
    ready = []
    for c, part in enumerate((own, other)):
        for d in range(4):
            for h in range(2):
                piece = part.at[jnp.where((s[0] >= d) == (h == 0), SLOT[d], SLOT[d + 4])]
                at = pl.ds((4 * c + d) * quarter, quarter), pl.ds(h * wide, wide)
                ready.append(copies.start(piece, passages.at[at]))
    for x in range(4):
        for h in range(2):
            for k in range(4):
                at = (h * 4 + k) * width
                queries[x * rows : (x + 1) * rows, at : at + width] = pieces[
                    x * 4 + (s[1] + 4 - k) % 4, h
                ]
    block = 2 * quarter
    wing = count // 2
    low, none = jnp.full((1, wing), -jnp.inf, F32), jnp.zeros((1, wing), F32)
    wait(ready)

    def chunk(k, found):
        fresh = []
        rows_at = pl.ds(pl.multiple_of(k * block, block), block)
        for j in range(2):
            at = slice(j * wing, (j + 1) * wing)
            values = dot(passages[rows_at], queries[at], ((1,), (1,))) * scale
            scores[rows_at, at] = values
            high, total = found[j]
            top = jnp.maximum(high, jnp.max(values, axis=0, keepdims=True))
            total = total * jnp.exp(high - top)
            fresh.append((top, total + jnp.sum(jnp.exp(values - top), axis=0, keepdims=True)))
        return tuple(fresh)

    found = lax.fori_loop(0, 4, chunk, ((low, none), (low, none)), unroll=UNROLL[0])
    for x in range(4):
        j, k = divmod(x, 2)
        at = slice(k * rows, (k + 1) * rows)
        stats[x : x + 1] = found[j][0][:, at]
        stats[4 + x : 5 + x] = found[j][1][:, at]


UNROLL = (1, True, 2)


def scored(scalars, own, other, pieces):
    _, _, rows, width = pieces.shape
    count, full, half = 4 * rows, 8 * width, 4 * own.shape[1]

    def body(*refs):
        score_body(*refs, scale=3.0 / math.sqrt(full))

    out = [near((count, full), BF16)]
    out += [near((2 * half, full), BF16), near((2 * half, count), F32), near((8, rows), F32)]
    return kernel(
        body, (scalars, own, other, pieces), "shhv", out, [], 16, 4 * half * count * full
    )


def grad_body(s, scores, *refs):
    seen, refs = refs[:4], refs[4:]
    queries, passages, d_own, d_other, terms, gv, bv, dv, tv, sems = refs
    half, count = scores.shape[0] // 2, scores.shape[1]
    full = queries.shape[1]
    block, quarter, rows, width = half // 2, half // 4, count // 4, full // 8
    logs, wanted = [], []
    for x in range(4):
        tops = [part[x : x + 1] for part in seen]
        top = functools.reduce(jnp.maximum, tops)
        total = sum(part[4 + x : 5 + x] * jnp.exp(high - top) for part, high in zip(seen, tops))
        logs.append(top + jnp.log(total))
        back = (s[10] + 4 - x) % 4
        wanted.append(sum(jnp.where(back == k, part[8:9], 0.0) for k, part in enumerate(seen)))
    log_total = jnp.concatenate(logs, axis=1)
    targets = jnp.concatenate(wanted, axis=1)

    def sent(source, b):
        target = (d_other, d_own)[source].at[pl.ds(b * block, block)]
        return pltpu.make_async_copy(dv.at[2 * source + b], target, sems.at[2 * source + b])

    def leaving(x, h, k):
        piece = terms.at[x * 4 + (s[1] + 4 - k) % 4, h]
        spot = tv.at[x, :, pl.ds((h * 4 + k) * width, width)]
        return pltpu.make_async_copy(spot, piece, sems.at[4 + 8 * x + 4 * h + k])

    for source in range(2):

        def one(b, _, source=source):
            for k in range(2):
                base = (1 - source) * half + b * block + k * quarter
                place = (1 - source) * 4 + 2 * b + k
                ids = s[2 + place] + lax.broadcasted_iota(jnp.int32, (quarter, 1), 0)
                hit = (ids.astype(F32) == targets).astype(F32)
                at = pl.ds(pl.multiple_of(base, quarter), quarter)
                value = (jnp.exp(scores[at] - log_total) - hit).astype(BF16)
                bv[k * quarter : (k + 1) * quarter] = value
                for x in range(4):
                    gv[x, at] = value[:, x * rows : (x + 1) * rows]
            dv[2 * source + b] = dot(bv[...], queries[...], ((1,), (0,)))
            sent(source, b).start()
            return 0

        lax.fori_loop(0, 2, one, 0, unroll=UNROLL[1])

    def another(x, _):
        tv[x] = dot(gv[x], passages[...], ((0,), (0,))).astype(BF16)
        for h in range(2):
            for k in range(4):
                leaving(x, h, k).start()
        return 0

    lax.fori_loop(0, 4, another, 0, unroll=UNROLL[2])
    for source in range(2):
        for b in range(2):
            sent(source, b).wait()
    for x in range(4):
        for h in range(2):
            for k in range(4):
                leaving(x, h, k).wait()


def gradients(scalars, scores, seen, queries, passages):
    half, count = scores.shape[0] // 2, scores.shape[1]
    full = queries.shape[1]
    out = [
        far((half, full), F32),
        far((half, full), F32),
        far((16, 2, count // 4, full // 8), BF16),
    ]
    scratch = [
        pltpu.VMEM((4, 2 * half, count // 4), BF16),
        pltpu.VMEM((half // 2, count), BF16),
        pltpu.VMEM((4, half // 2, full), F32),
        pltpu.VMEM((4, count // 4, full), BF16),
    ]
    args = (scalars, scores, *seen, queries, passages)
    return kernel(grad_body, args, "s" + 7 * "v", out, scratch, 40, 8 * half * count * full)


def combine_body(s, own, theirs, *refs):
    outs, (av, bv, fv, ov, sems) = refs[:9], refs[9:]
    quarter, wide = outs[0].shape
    half = quarter // 2
    copies = Copies(sems)
    order = (3, 0, 2, 1)
    loads = {}
    for d in order:
        at = pl.ds(d * quarter, quarter)
        loads[d] = (
            copies.start(own.at[at], av.at[at]),
            copies.start(theirs.at[at], bv.at[at]),
        )
    ends = []
    for d in order:
        wait(loads[d])
        at = slice(d * quarter, (d + 1) * quarter)
        pair = av[at] + bv[at]
        left, right = pair[:, :wide], pair[:, wide:]
        here = s[0] >= d
        for k, value in ((d, jnp.where(here, left, right)), (d + 4, jnp.where(here, right, left))):
            if k in (0, 1, 7):
                place = (0, 1, 7).index(k)
                fv[place] = value
                ends.append(copies.start(fv.at[place], outs[place]))
                continue
            ov[k - 2] = value.astype(BF16)
            if k == 4:
                ends.append(copies.start(ov.at[2, pl.ds(0, half)], outs[7]))
                ends.append(copies.start(ov.at[2, pl.ds(half, half)], outs[8]))
            else:
                ends.append(copies.start(ov.at[k - 2], outs[3 + (2, 3, 5, 6).index(k)]))
    wait(ends)


def combined(scalars, own, theirs):
    rows, full = own.shape
    quarter, wide = rows // 4, full // 2
    scratch = [
        pltpu.VMEM((rows, full), F32),
        pltpu.VMEM((rows, full), F32),
        pltpu.VMEM((3, quarter, wide), F32),
        pltpu.VMEM((5, quarter, wide), BF16),
    ]
    out = [far((quarter, wide), F32)] * 3 + [far((quarter, wide), BF16)] * 4
    out += [far((quarter // 2, wide), BF16)] * 2
    return kernel(combine_body, (scalars, own, theirs), "shh", out, scratch, 17, 2**31)


def local(queries, passages, positive):
    return step(queries, passages, positive)


def step(queries, passages, positive):
    rows, width = queries.shape
    half, quarter = rows // 2, rows // 4
    x, y, c = (lax.axis_index(a) for a in ("x", "y", "c"))
    zl, zh = lax.axis_index("zl"), lax.axis_index("zh")

    kept = lax.dynamic_slice(queries, (zh * half, 0), (half, width))
    sent = lax.dynamic_slice(queries, ((1 - zh) * half, 0), (half, width))
    copies = copies_of(swapped(sent, "zh"), 1, copies_of(kept, 0))
    pieces = lax.all_to_all(copies, PLANE, 0, 0, tiled=True)

    mine = [
        lax.dynamic_slice(passages, ((y + d) % 4 * quarter, 0), (quarter, width)) for d in range(4)
    ]
    crossed = [along(mine[d], "y", d) for d in (1, 2, 3)]
    passage_part = jnp.concatenate([mine[0], *crossed], axis=1)
    own = ring_gather(passage_part).reshape(8, quarter, 4 * width)
    other = swapped(own, "c")

    source_c = jnp.stack([c, 1 - c])
    group = (((zl - jnp.arange(4)) % 4) * 4 + x)[None, :] * 2 + source_c[:, None]
    first = (group * rows + y * quarter).reshape(8)
    scalars = jnp.concatenate([zl[None], y[None], first, x[None]]).astype(jnp.int32)

    block_queries, block_passages, scores, stats = scored(scalars, own, other, pieces)
    wanted = lax.dynamic_slice(positive, (zh * half,), (half,)).astype(F32)
    seen = [stats] + [along(stats, "y", d) for d in (1, 2, 3)]
    tops = functools.reduce(jnp.maximum, [part[:4] for part in seen])
    totals = sum(part[4:] * jnp.exp(part[:4] - tops) for part in seen)
    stats = jnp.concatenate([tops, totals, wanted[None]])
    seen = [stats] + [along(stats, "x", d) for d in (1, 2, 3)]

    d_own, d_other, terms = gradients(scalars, scores, seen, block_queries, block_passages)
    theirs = swapped(d_other, "c")
    terms = lax.all_to_all(terms, PLANE, 0, 0, tiled=True)
    mine, down, up, d2, d3, d5, d6, low, high = combined(scalars, d_own, theirs)
    low, high = along_z(low, -3), along_z(high, 3)
    d3, d5 = along_z(d3, -2), along_z(d5, 2)
    d2, d6 = along_z(d2, -2), along_z(d6, 2)
    rest, rest_up = ((0, quarter // 2), (0, 0)), ((quarter // 2, 0), (0, 0))
    down = (down + d3.astype(F32) + jnp.pad(low.astype(F32), rest)).astype(BF16)
    up = (up + d5.astype(F32) + jnp.pad(high.astype(F32), rest_up)).astype(BF16)
    down, up = along_z(down, -1), along_z(up, 1)
    total = mine
    for part in (d2, d6, down, up):
        total += part.astype(F32)
    total = total.astype(BF16)
    slices = [total[:, k * width : (k + 1) * width] for k in range(4)]
    slices = [slices[0]] + [along(slices[k], "y", -k) for k in (1, 2, 3)]
    grad_passages = jnp.concatenate(
        [lax.select_n((q + 4 - y) % 4, *slices) for q in range(4)]
    )

    grad_queries = jnp.sum(terms.astype(F32), axis=0).astype(BF16)
    kept, received = grad_queries[0], swapped(grad_queries[1], "zh")
    grad_queries = jnp.where(
        zh == 0, jnp.concatenate([kept, received]), jnp.concatenate([received, kept])
    )
    return grad_queries, grad_passages


def solution(mesh):
    finer = Mesh(mesh.devices.reshape(4, 4, 2, 2, 4), ("zl", "x", "c", "zh", "y"))
    groups = ("zl", "x", "c")
    return jax.shard_map(
        step if INTERPRET else local,
        mesh=finer,
        in_specs=(P(groups, WIDTH), P(groups, WIDTH), P(groups)),
        out_specs=(P(groups, WIDTH), P(groups, WIDTH)),
        check_vma=False,
    )
```

```python
import functools
import math

import jax
import jax.numpy as jnp
from jax import lax
from jax.experimental import pallas as pl
from jax.experimental.pallas import tpu as pltpu
from jax.sharding import Mesh
from jax.sharding import PartitionSpec as P

WIDTH = ("zh", "y")
PLANE = ("x", "y")
F32, BF16 = jnp.float32, jnp.bfloat16
INTERPRET = False


def along_z(array, step):
    place = lambda z: (z % 4) * 2 + z // 4
    return lax.ppermute(array, ("zl", "zh"), [(place(z), place((z + step) % 8)) for z in range(8)])


def along(array, axis, step):
    return lax.ppermute(array, axis, [(k, (k + step) % 4) for k in range(4)])


def swapped(array, axis):
    return lax.ppermute(array, axis, [(0, 1), (1, 0)])


def dot(a, b, dims):
    return lax.dot_general(a, b, (dims, ((), ())), preferred_element_type=F32)


def ring_gather(piece):
    half = piece.shape[0] // 2
    down, up = [piece], [piece]
    for _ in range(3):
        down.append(along_z(down[-1], 1))
        up.append(along_z(up[-1], -1))
    far = jnp.concatenate([along_z(down[3][:half], 1), along_z(up[3][half:], -1)])
    return jnp.concatenate([piece, down[1], up[1], down[2], up[2], down[3], up[3], far])


SLOT = (0, 1, 3, 5, 7, 6, 4, 2)


def kernel(body, args, places, out_shape, scratch, copies, flops, aliases=None):
    hbm, vmem = pl.BlockSpec(memory_space=pl.ANY), pl.BlockSpec(memory_space=pltpu.VMEM)
    if not INTERPRET:
        args = [
            a
            if p == "s"
            else pltpu.with_memory_space_constraint(a, pltpu.VMEM if p == "v" else pltpu.HBM)
            for a, p in zip(args, places)
        ]
    spec_of = {"v": vmem, "h": hbm, "s": pl.BlockSpec(memory_space=pltpu.SMEM)}
    return pl.pallas_call(
        body,
        in_specs=[spec_of[p] for p in places],
        out_specs=[vmem if o.near else hbm for o in out_shape],
        out_shape=[o.placed() for o in out_shape],
        scratch_shapes=[*scratch, pltpu.SemaphoreType.DMA((copies,))],
        compiler_params=pltpu.CompilerParams(vmem_limit_bytes=26 * 2**20),
        cost_estimate=pl.CostEstimate(
            flops=flops, transcendentals=0, bytes_accessed=flops // 512
        ),
        input_output_aliases=aliases or {},
        interpret=INTERPRET,
    )(*args)


class Out:
    def __init__(self, near, shape, dtype):
        self.near, self.shape, self.dtype = near, shape, dtype

    def placed(self):
        if INTERPRET:
            return jax.ShapeDtypeStruct(self.shape, self.dtype)
        return (pltpu.VMEM if self.near else pltpu.HBM)(self.shape, self.dtype)


near = functools.partial(Out, True)
far = functools.partial(Out, False)


class Copies:
    def __init__(self, sems):
        self.sems, self.used = sems, 0

    def start(self, source, target):
        copy = pltpu.make_async_copy(source, target, self.sems.at[self.used])
        self.used += 1
        copy.start()
        return copy


def wait(copies):
    for copy in copies:
        copy.wait()


def copies_of(array, place, before=None):
    def body(source, *refs):
        *_, out, sems = refs
        copies = Copies(sems)
        wait([copies.start(source, out.at[n, place]) for n in range(16)])

    args = (array,) if before is None else (array, before)
    out = [far((16, 2, *array.shape), array.dtype)]
    aliases = None if before is None else {1: 0}
    return kernel(body, args, "vh"[: len(args)], out, [], 16, 2**24, aliases)[0]


def score_body(s, own, other, pieces, queries, passages, scores, stats, sems, *, scale):
    _, quarter, wide = own.shape
    count, full = queries.shape
    rows, width = count // 4, full // 8
    copies = Copies(sems)
    ready = []
    for c, part in enumerate((own, other)):
        for d in range(4):
            for h in range(2):
                piece = part.at[jnp.where((s[0] >= d) == (h == 0), SLOT[d], SLOT[d + 4])]
                at = pl.ds((4 * c + d) * quarter, quarter), pl.ds(h * wide, wide)
                ready.append(copies.start(piece, passages.at[at]))
    for x in range(4):
        for h in range(2):
            for k in range(4):
                at = (h * 4 + k) * width
                queries[x * rows : (x + 1) * rows, at : at + width] = pieces[
                    x * 4 + (s[1] + 4 - k) % 4, h
                ]
    block = 2 * quarter
    wing = count // 2
    low, none = jnp.full((1, wing), -jnp.inf, F32), jnp.zeros((1, wing), F32)
    wait(ready)

    def chunk(k, found):
        fresh = []
        rows_at = pl.ds(pl.multiple_of(k * block, block), block)
        for j in range(2):
            at = slice(j * wing, (j + 1) * wing)
            values = dot(passages[rows_at], queries[at], ((1,), (1,))) * scale
            scores[rows_at, at] = values
            high, total = found[j]
            top = jnp.maximum(high, jnp.max(values, axis=0, keepdims=True))
            total = total * jnp.exp(high - top)
            fresh.append((top, total + jnp.sum(jnp.exp(values - top), axis=0, keepdims=True)))
        return tuple(fresh)

    found = lax.fori_loop(0, 4, chunk, ((low, none), (low, none)), unroll=UNROLL[0])
    for x in range(4):
        j, k = divmod(x, 2)
        at = slice(k * rows, (k + 1) * rows)
        stats[x : x + 1] = found[j][0][:, at]
        stats[4 + x : 5 + x] = found[j][1][:, at]


UNROLL = (2, True, 2)


def scored(scalars, own, other, pieces):
    _, _, rows, width = pieces.shape
    count, full, half = 4 * rows, 8 * width, 4 * own.shape[1]

    def body(*refs):
        score_body(*refs, scale=3.0 / math.sqrt(full))

    out = [near((count, full), BF16)]
    out += [near((2 * half, full), BF16), near((2 * half, count), F32), near((8, rows), F32)]
    return kernel(
        body, (scalars, own, other, pieces), "shhv", out, [], 16, 4 * half * count * full
    )


def grad_body(s, scores, *refs):
    seen, refs = refs[:4], refs[4:]
    queries, passages, d_own, d_other, terms, gv, bv, dv, tv, sems = refs
    half, count = scores.shape[0] // 2, scores.shape[1]
    full = queries.shape[1]
    block, quarter, rows, width = half // 2, half // 4, count // 4, full // 8
    logs, wanted = [], []
    for x in range(4):
        tops = [part[x : x + 1] for part in seen]
        top = functools.reduce(jnp.maximum, tops)
        total = sum(part[4 + x : 5 + x] * jnp.exp(high - top) for part, high in zip(seen, tops))
        logs.append(top + jnp.log(total))
        back = (s[10] + 4 - x) % 4
        wanted.append(sum(jnp.where(back == k, part[8:9], 0.0) for k, part in enumerate(seen)))
    log_total = jnp.concatenate(logs, axis=1)
    targets = jnp.concatenate(wanted, axis=1)

    def sent(source, b):
        target = (d_other, d_own)[source].at[pl.ds(b * block, block)]
        return pltpu.make_async_copy(dv.at[2 * source + b], target, sems.at[2 * source + b])

    def leaving(x, h, k):
        piece = terms.at[x * 4 + (s[1] + 4 - k) % 4, h]
        spot = tv.at[x, :, pl.ds((h * 4 + k) * width, width)]
        return pltpu.make_async_copy(spot, piece, sems.at[4 + 8 * x + 4 * h + k])

    for source in range(2):

        def one(b, _, source=source):
            for k in range(2):
                base = (1 - source) * half + b * block + k * quarter
                place = (1 - source) * 4 + 2 * b + k
                ids = s[2 + place] + lax.broadcasted_iota(jnp.int32, (quarter, 1), 0)
                hit = (ids.astype(F32) == targets).astype(F32)
                at = pl.ds(pl.multiple_of(base, quarter), quarter)
                value = (jnp.exp(scores[at] - log_total) - hit).astype(BF16)
                bv[k * quarter : (k + 1) * quarter] = value
                for x in range(4):
                    gv[x, at] = value[:, x * rows : (x + 1) * rows]
            dv[2 * source + b] = dot(bv[...], queries[...], ((1,), (0,)))
            sent(source, b).start()
            return 0

        lax.fori_loop(0, 2, one, 0, unroll=UNROLL[1])

    def another(x, _):
        tv[x] = dot(gv[x], passages[...], ((0,), (0,))).astype(BF16)
        for h in range(2):
            for k in range(4):
                leaving(x, h, k).start()
        return 0

    lax.fori_loop(0, 4, another, 0, unroll=UNROLL[2])
    for source in range(2):
        for b in range(2):
            sent(source, b).wait()
    for x in range(4):
        for h in range(2):
            for k in range(4):
                leaving(x, h, k).wait()


def gradients(scalars, scores, seen, queries, passages):
    half, count = scores.shape[0] // 2, scores.shape[1]
    full = queries.shape[1]
    out = [
        far((half, full), F32),
        far((half, full), F32),
        far((16, 2, count // 4, full // 8), BF16),
    ]
    scratch = [
        pltpu.VMEM((4, 2 * half, count // 4), BF16),
        pltpu.VMEM((half // 2, count), BF16),
        pltpu.VMEM((4, half // 2, full), F32),
        pltpu.VMEM((4, count // 4, full), BF16),
    ]
    args = (scalars, scores, *seen, queries, passages)
    return kernel(grad_body, args, "s" + 7 * "v", out, scratch, 40, 8 * half * count * full)


def combine_body(s, own, theirs, *refs):
    outs, (av, bv, fv, ov, sems) = refs[:9], refs[9:]
    quarter, wide = outs[0].shape
    half = quarter // 2
    copies = Copies(sems)
    order = (3, 0, 2, 1)
    loads = {}
    for d in order:
        at = pl.ds(d * quarter, quarter)
        loads[d] = (
            copies.start(own.at[at], av.at[at]),
            copies.start(theirs.at[at], bv.at[at]),
        )
    ends = []
    for d in order:
        wait(loads[d])
        at = slice(d * quarter, (d + 1) * quarter)
        pair = av[at] + bv[at]
        left, right = pair[:, :wide], pair[:, wide:]
        here = s[0] >= d
        for k, value in ((d, jnp.where(here, left, right)), (d + 4, jnp.where(here, right, left))):
            if k in (0, 1, 7):
                place = (0, 1, 7).index(k)
                fv[place] = value
                ends.append(copies.start(fv.at[place], outs[place]))
                continue
            ov[k - 2] = value.astype(BF16)
            if k == 4:
                ends.append(copies.start(ov.at[2, pl.ds(0, half)], outs[7]))
                ends.append(copies.start(ov.at[2, pl.ds(half, half)], outs[8]))
            else:
                ends.append(copies.start(ov.at[k - 2], outs[3 + (2, 3, 5, 6).index(k)]))
    wait(ends)


def combined(scalars, own, theirs):
    rows, full = own.shape
    quarter, wide = rows // 4, full // 2
    scratch = [
        pltpu.VMEM((rows, full), F32),
        pltpu.VMEM((rows, full), F32),
        pltpu.VMEM((3, quarter, wide), F32),
        pltpu.VMEM((5, quarter, wide), BF16),
    ]
    out = [far((quarter, wide), F32)] * 3 + [far((quarter, wide), BF16)] * 4
    out += [far((quarter // 2, wide), BF16)] * 2
    return kernel(combine_body, (scalars, own, theirs), "shh", out, scratch, 17, 2**31)


def local(queries, passages, positive):
    return step(queries, passages, positive)


def step(queries, passages, positive):
    rows, width = queries.shape
    half, quarter = rows // 2, rows // 4
    x, y, c = (lax.axis_index(a) for a in ("x", "y", "c"))
    zl, zh = lax.axis_index("zl"), lax.axis_index("zh")

    kept = lax.dynamic_slice(queries, (zh * half, 0), (half, width))
    sent = lax.dynamic_slice(queries, ((1 - zh) * half, 0), (half, width))
    copies = copies_of(swapped(sent, "zh"), 1, copies_of(kept, 0))
    pieces = lax.all_to_all(copies, PLANE, 0, 0, tiled=True)

    mine = [
        lax.dynamic_slice(passages, ((y + d) % 4 * quarter, 0), (quarter, width)) for d in range(4)
    ]
    crossed = [along(mine[d], "y", d) for d in (1, 2, 3)]
    passage_part = jnp.concatenate([mine[0], *crossed], axis=1)
    own = ring_gather(passage_part).reshape(8, quarter, 4 * width)
    other = swapped(own, "c")

    source_c = jnp.stack([c, 1 - c])
    group = (((zl - jnp.arange(4)) % 4) * 4 + x)[None, :] * 2 + source_c[:, None]
    first = (group * rows + y * quarter).reshape(8)
    scalars = jnp.concatenate([zl[None], y[None], first, x[None]]).astype(jnp.int32)

    block_queries, block_passages, scores, stats = scored(scalars, own, other, pieces)
    wanted = lax.dynamic_slice(positive, (zh * half,), (half,)).astype(F32)
    seen = [stats] + [along(stats, "y", d) for d in (1, 2, 3)]
    tops = functools.reduce(jnp.maximum, [part[:4] for part in seen])
    totals = sum(part[4:] * jnp.exp(part[:4] - tops) for part in seen)
    stats = jnp.concatenate([tops, totals, wanted[None]])
    seen = [stats] + [along(stats, "x", d) for d in (1, 2, 3)]

    d_own, d_other, terms = gradients(scalars, scores, seen, block_queries, block_passages)
    theirs = swapped(d_other, "c")
    terms = lax.all_to_all(terms, PLANE, 0, 0, tiled=True)
    mine, down, up, d2, d3, d5, d6, low, high = combined(scalars, d_own, theirs)
    low, high = along_z(low, -3), along_z(high, 3)
    d3, d5 = along_z(d3, -2), along_z(d5, 2)
    d2, d6 = along_z(d2, -1), along_z(d6, 1)
    rest, rest_up = ((0, quarter // 2), (0, 0)), ((quarter // 2, 0), (0, 0))
    low, high = jnp.pad(low, rest), jnp.pad(high, rest_up)
    down = sum(part.astype(F32) for part in (d2, d3, low)) + down
    up = sum(part.astype(F32) for part in (d6, d5, high)) + up
    down, up = down.astype(BF16), up.astype(BF16)
    down, up = along_z(down, -1), along_z(up, 1)
    total = mine
    for part in (down, up):
        total += part.astype(F32)
    total = total.astype(BF16)
    slices = [total[:, k * width : (k + 1) * width] for k in range(4)]
    slices = [slices[0]] + [along(slices[k], "y", -k) for k in (1, 2, 3)]
    grad_passages = jnp.concatenate(
        [lax.select_n((q + 4 - y) % 4, *slices) for q in range(4)]
    )

    grad_queries = jnp.sum(terms.astype(F32), axis=0).astype(BF16)
    kept, received = grad_queries[0], swapped(grad_queries[1], "zh")
    grad_queries = jnp.where(
        zh == 0, jnp.concatenate([kept, received]), jnp.concatenate([received, kept])
    )
    return grad_queries, grad_passages


def solution(mesh):
    finer = Mesh(mesh.devices.reshape(4, 4, 2, 2, 4), ("zl", "x", "c", "zh", "y"))
    groups = ("zl", "x", "c")
    return jax.shard_map(
        step if INTERPRET else local,
        mesh=finer,
        in_specs=(P(groups, WIDTH), P(groups, WIDTH), P(groups)),
        out_specs=(P(groups, WIDTH), P(groups, WIDTH)),
        check_vma=False,
    )
```
